8 devices in a mesh: dp: 2 (over z, y), ep: 4 (over x, core).
Axes of the slice: x: 2, y: 2, z: 1, core: 2. Of those that a mesh axis runs over, the one named last changes fastest.
Arguments:
- x_tokens: bfloat16 [512, 1024], P(('dp', 'ep')), parts along dimension 0
- dy_tokens: bfloat16 [512, 1024], P(('dp', 'ep')), parts along dimension 0
- expert_ids: int32 [512, 8], P(('dp', 'ep')), parts along dimension 0
- gate_vals: float32 [512, 8], P(('dp', 'ep')), parts along dimension 0
- slot_ids: int32 [512, 8], P(('dp', 'ep')), parts along dimension 0
- w_gate: bfloat16 [32, 1024, 512], P('ep')
- w_down: bfloat16 [32, 512, 1024], P('ep')
- w_up: bfloat16 [32, 1024, 512], P('ep')
Outputs:
- output 1: bfloat16 [512, 1024], P(('dp', 'ep')), parts along dimension 0
- output 2: float32 [64, 1024, 512], P(('dp', 'ep')), parts along dimension 0
- output 3: float32 [64, 512, 1024], P(('dp', 'ep')), parts along dimension 0
- output 4: float32 [64, 1024, 512], P(('dp', 'ep')), parts along dimension 0
There are 2 independent parts. The reference program is written for one: setup_inputs(seed, part) draws one part's arguments, and reference() takes and returns one part's arrays. A program takes and returns all parts, laid end to end along the dimension named above; an argument that names none is the same for every part.
All inputs are finite; a program needn't handle non-finite values.
Results may differ from the reference program's by a relative error of at most 0.0103763.
Values are sent between devices in bfloat16 or wider.
A program may use at most 1 GiB of HBM per device.

```python
import jax
import jax.numpy as jnp
from jax import lax

D = 1024
FF = 512
EXPERTS = 32
TOP = 8
GROUP = 4
TOK = 64
CAP = 24


def source_routing(src_key):
    key_base, key_offset, key_hot = jax.random.split(src_key, 3)
    stride = EXPERTS // TOP
    base_expert = jax.random.randint(key_base, (TOK,), 0, EXPERTS)
    offset = jax.random.randint(key_offset, (TOK, TOP), 0, stride)
    hot_expert = jax.random.randint(key_hot, (), 0, EXPERTS)
    forced = jnp.arange(TOK) < CAP
    base_expert = jnp.where(forced, hot_expert, base_expert)
    offset = jnp.where(forced[:, None] & (jnp.arange(TOP)[None, :] == 0), 0, offset)
    experts = (base_expert[:, None] + jnp.arange(TOP)[None, :] * stride + offset) % EXPERTS
    n_copy = TOK * TOP
    flat_exp = experts.reshape(n_copy)
    copy_ids = jnp.arange(n_copy)
    sort_order = jnp.argsort(flat_exp * n_copy + copy_ids)
    exp_counts = jnp.zeros((EXPERTS,), jnp.int32).at[flat_exp].add(1)
    exp_starts = jnp.cumsum(exp_counts) - exp_counts
    sorted_rank = copy_ids - exp_starts[flat_exp[sort_order]]
    copy_rank = jnp.zeros((n_copy,), jnp.int32).at[sort_order].set(sorted_rank)
    slots = jnp.where(copy_rank < CAP, copy_rank, -1)
    return experts.astype(jnp.int32), slots.reshape(TOK, TOP).astype(jnp.int32)


def setup_inputs(seed: int = 0, part: int = 0) -> dict:
    root_key = jax.random.key(seed)
    sub_keys = jax.random.split(root_key, 7)
    n_tok = GROUP * TOK
    x_tokens = jax.random.normal(jax.random.fold_in(sub_keys[0], part), (n_tok, D), jnp.float32).astype(jnp.bfloat16)
    dy_tokens = jax.random.normal(jax.random.fold_in(sub_keys[1], part), (n_tok, D), jnp.float32).astype(jnp.bfloat16)
    gate_vals = jax.random.uniform(jax.random.fold_in(sub_keys[2], part), (n_tok, TOP), jnp.float32, 0.3, 1.0)
    src_keys = jax.random.split(jax.random.fold_in(sub_keys[3], part), GROUP)
    expert_ids, slot_ids = jax.vmap(source_routing)(src_keys)
    w_gate = (jax.random.normal(sub_keys[4], (EXPERTS, D, FF), jnp.float32) * D ** -0.5).astype(jnp.bfloat16)
    w_down = (jax.random.normal(sub_keys[5], (EXPERTS, FF, D), jnp.float32) * FF ** -0.5).astype(jnp.bfloat16)
    w_up = (jax.random.normal(sub_keys[6], (EXPERTS, D, FF), jnp.float32) * D ** -0.5).astype(jnp.bfloat16)
    return {'x_tokens': x_tokens, 'dy_tokens': dy_tokens, 'expert_ids': expert_ids.reshape(n_tok, TOP), 'gate_vals': gate_vals, 'slot_ids': slot_ids.reshape(n_tok, TOP), 'w_gate': w_gate, 'w_down': w_down, 'w_up': w_up}


def expert_backward(operands):
    x_rows, dz_rows, w_gate, w_down, w_up = operands
    a_pre = jnp.dot(x_rows, w_gate, preferred_element_type=jnp.float32).astype(jnp.bfloat16).astype(jnp.float32)
    b_pre = jnp.dot(x_rows, w_up, preferred_element_type=jnp.float32).astype(jnp.bfloat16).astype(jnp.float32)
    sigma_a = jax.nn.sigmoid(a_pre)
    silu_a = a_pre * sigma_a
    hidden = (silu_a * b_pre).astype(jnp.bfloat16)
    d_hidden = jnp.dot(dz_rows, w_down.T, preferred_element_type=jnp.float32)
    d_gate = (d_hidden * b_pre * sigma_a * (1.0 + a_pre * (1.0 - sigma_a))).astype(jnp.bfloat16)
    d_up = (d_hidden * silu_a).astype(jnp.bfloat16)
    g_down = jnp.dot(hidden.T, dz_rows, preferred_element_type=jnp.float32)
    g_gate = jnp.dot(x_rows.T, d_gate, preferred_element_type=jnp.float32)
    g_up = jnp.dot(x_rows.T, d_up, preferred_element_type=jnp.float32)
    dx_rows = (jnp.dot(d_gate, w_gate.T, preferred_element_type=jnp.float32) + jnp.dot(d_up, w_up.T, preferred_element_type=jnp.float32)).astype(jnp.bfloat16)
    return dx_rows, g_gate, g_down, g_up


def reference(x_tokens, dy_tokens, expert_ids, gate_vals, slot_ids, w_gate, w_down, w_up):
    n_tok = GROUP * TOK
    n_rows = GROUP * CAP
    n_slot = EXPERTS * n_rows
    source = jnp.arange(n_tok) // TOK
    buf_index = jnp.where(slot_ids >= 0, expert_ids * n_rows + source[:, None] * CAP + slot_ids, n_slot)
    slot_copy = jnp.full((n_slot,), n_tok * TOP, jnp.int32).at[buf_index.reshape(n_tok * TOP)].set(jnp.arange(n_tok * TOP, dtype=jnp.int32), mode='drop')
    slot_tok = slot_copy // TOP
    x_buf = jnp.take(x_tokens, slot_tok, axis=0, mode='fill', fill_value=0).reshape(EXPERTS, n_rows, D)
    gate_slot = jnp.take(gate_vals.reshape(n_tok * TOP), slot_copy, mode='fill', fill_value=0)
    dy_slot = jnp.take(dy_tokens, slot_tok, axis=0, mode='fill', fill_value=0)
    dz_buf = (gate_slot[:, None] * dy_slot).astype(jnp.bfloat16).reshape(EXPERTS, n_rows, D)
    dx_buf, dw_gate, dw_down, dw_up = lax.map(expert_backward, (x_buf, dz_buf, w_gate, w_down, w_up))
    returned = jnp.take(dx_buf.reshape(n_slot, D), buf_index, axis=0, mode='fill', fill_value=0)
    dx_tokens = jnp.sum(returned.astype(jnp.float32), axis=1).astype(jnp.bfloat16)
    return (dx_tokens, dw_gate, dw_down, dw_up)
```

```python
import functools

import jax
import jax.numpy as jnp
from jax import lax
from jax.experimental import pallas as pl
from jax.experimental.pallas import tpu as pltpu
from jax.sharding import PartitionSpec as P

MESH = pl.DeviceIdType.MESH
F32 = jnp.float32
BF16 = jnp.bfloat16
NN = (((1,), (0,)), ((), ()))
NT = (((1,), (1,)), ((), ()))
TN = (((0,), (0,)), ((), ()))


def slot_capacity(tok_dev, top_k, n_exp):
    return ((3 * tok_dev * top_k) // (2 * n_exp) + 7) // 8 * 8


def mm(a, b, dims):
    return lax.dot_general(a, b, dims, preferred_element_type=F32)


def peers():
    ep = lax.axis_index('ep')
    core = lax.rem(ep, 2)
    chip = ep - core
    mate = chip + 1 - core
    far = lax.rem(ep + 2, 4)
    far_mate = lax.rem(mate + 2, 4)
    return ep, mate, far, far_mate


def entry_barrier(others):
    barrier = pltpu.get_barrier_semaphore()
    for other in others:
        pl.semaphore_signal(barrier, inc=1, device_id={'ep': other}, device_id_type=MESH)
    pl.semaphore_wait(barrier, len(others))


def gather_kernel(cap, x_hbm, dy_hbm, ids_hbm, slot_hbm, gate_hbm, w1_hbm, w3_hbm, w2_hbm, xg, dyg, metag, w1, w3, w2, x_ref, dy_ref, ids_ref, slot_ref, gate_ref, meta, w_sem, loc_sem, send_sem, recv_sem):
    ep, mate, far, far_mate = peers()
    n_local = w1.shape[0]
    tok = x_ref.shape[0]
    small = []
    for k, (src, dst) in enumerate(((x_hbm, x_ref), (dy_hbm, dy_ref), (ids_hbm, ids_ref), (slot_hbm, slot_ref), (gate_hbm, gate_ref))):
        c = pltpu.make_async_copy(src, dst, loc_sem.at[k])
        c.start()
        small.append(c)
    copies = []
    for e in range(n_local):
        for k, (src, dst) in enumerate(((w1_hbm, w1), (w3_hbm, w3), (w2_hbm, w2))):
            c = pltpu.make_async_copy(src.at[e], dst.at[e], w_sem.at[k, e])
            c.start()
            copies.append(c)
    meta[...] = jnp.zeros_like(meta)
    for c in small:
        c.wait()
    key = jnp.where(slot_ref[...] >= 0, ids_ref[...] * cap + slot_ref[...], -1)
    meta[0:8, 0:tok] = key.astype(F32)
    meta[8:16, 0:tok] = gate_ref[...]
    entry_barrier((mate, far, far_mate))
    remote = []

    def send(src, dst, k, to):
        c = pltpu.make_async_remote_copy(src_ref=src, dst_ref=dst, send_sem=send_sem.at[k], recv_sem=recv_sem.at[k], device_id={'ep': to}, device_id_type=MESH)
        c.start()
        remote.append(c)
        return c

    half = tok // 2
    mine = pl.multiple_of(ep * tok, tok)
    pieces = [(src, dst, h * half) for src, dst in ((x_ref, xg), (dy_ref, dyg)) for h in range(2)]
    from_far = []
    for k, (src, dst, off) in enumerate(pieces):
        from_far.append(send(src.at[pl.ds(off, half)], dst.at[pl.ds(mine + off, half)], k, far))
    for k, (src, dst, off) in enumerate(pieces):
        send(src.at[pl.ds(off, half)], dst.at[pl.ds(mine + off, half)], 4 + k, mate)
    for k, to in enumerate((far, mate, far_mate)):
        send(meta, metag.at[ep], 12 + k, to)
    xg[pl.ds(mine, tok), :] = x_ref[...]
    dyg[pl.ds(mine, tok), :] = dy_ref[...]
    metag[ep] = meta[...]
    theirs = pl.multiple_of(far * tok, tok)
    for k, (src, dst, off) in enumerate(pieces):
        from_far[k].wait_recv()
        here = dst.at[pl.ds(theirs + off, half)]
        send(here, here, 8 + k, mate)
    for c in from_far:
        c.wait_send()
    for c in remote[4:]:
        c.wait()
    for c in copies:
        c.wait()


def expert_kernel(cap, n_src, xg, dyg, metag, w1, w3, w2, g1, g3, g2, part, p_all, x_all, dz_all, dx_all, s1, s3, s2, out_sem):
    ep = lax.axis_index('ep')
    n_local = w1.shape[0]
    rows = n_src * cap
    n_tok = xg.shape[0]
    tok = n_tok // n_src
    halves = []
    for pair in range(n_src // 2):
        halves.append(metag[2 * pair] + pltpu.roll(metag[2 * pair + 1], tok, 1))
    meta = jnp.concatenate(halves, axis=1)
    key = meta[0:8, :].astype(jnp.int32)
    gate = meta[8:16, :]
    lane = lax.broadcasted_iota(jnp.int32, (1, n_tok), 1)
    src_base = (lane // tok) * cap
    row_id = lax.broadcasted_iota(jnp.int32, (rows, n_tok), 0)

    def dispatch(e):
        lo = (ep * n_local + e) * cap
        hit = (key >= lo) & (key < lo + cap)
        slot = jnp.sum(jnp.where(hit, key - lo + 1, 0), axis=0, keepdims=True)
        g_tok = jnp.sum(jnp.where(hit, gate, 0.0), axis=0, keepdims=True)
        want = jnp.where(slot > 0, slot - 1 + src_base, -1)
        pick = row_id == want
        g_row = jnp.sum(jnp.where(pick, g_tok, 0.0), axis=1, keepdims=True)
        sel = jnp.where(pick, 1.0, 0.0).astype(BF16)
        p_all[e] = sel
        x_rows = mm(sel, xg[...], NN).astype(BF16)
        dy_rows = mm(sel, dyg[...], NN)
        x_all[e] = x_rows
        dz_all[e] = (g_row * dy_rows).astype(BF16)

    def copies(e, slot):
        return [pltpu.make_async_copy(s.at[slot], g.at[e], out_sem.at[k, slot]) for k, (s, g) in enumerate(((s1, g1), (s3, g3), (s2, g2)))]

    def step(e, carry):
        slot = lax.rem(e, 2)

        @pl.when(e >= 2)
        def _():
            for c in copies(e - 2, slot):
                c.wait()

        dispatch(e)
        x_rows = x_all[e]
        dz_rows = dz_all[e]
        a = mm(x_rows, w1[e], NN).astype(BF16).astype(F32)
        b = mm(x_rows, w3[e], NN).astype(BF16).astype(F32)
        dh = mm(dz_rows, w2[e], NT)
        sg = jax.nn.sigmoid(a)
        silu = a * sg
        h = (silu * b).astype(BF16)
        da = (dh * b * sg * (1.0 + a * (1.0 - sg))).astype(BF16)
        db = (dh * silu).astype(BF16)
        dx_all[e] = (mm(da, w1[e], NT) + mm(db, w3[e], NT)).astype(BF16)
        s2[slot] = mm(h, dz_rows, TN)
        s1[slot] = mm(x_rows, da, TN)
        s3[slot] = mm(x_rows, db, TN)
        for c in copies(e, slot):
            c.start()
        return carry

    lax.fori_loop(0, n_local, step, 0)
    total = mm(p_all[...].reshape(n_local * rows, n_tok), dx_all[...].reshape(n_local * rows, -1), TN)
    for s in range(n_src):
        part[s] = total[s * tok:(s + 1) * tok]
    for e in (n_local - 2, n_local - 1):
        for c in copies(e, e % 2):
            c.wait()


def reduce_kernel(part, dx_ref, got, pair, far_got, send_sem, recv_sem):
    ep, mate, far, far_mate = peers()
    entry_barrier((mate, far))
    tok = part.shape[1]
    n_chunk = 4
    q = tok // n_chunk

    def send(src, dst, k, to):
        c = pltpu.make_async_remote_copy(src_ref=src, dst_ref=dst, send_sem=send_sem.at[k], recv_sem=recv_sem.at[k], device_id={'ep': to}, device_id_type=MESH)
        c.start()
        return c

    first = []
    for i in range(n_chunk):
        first.append(send(part.at[far_mate, pl.ds(i * q, q)], got.at[0, pl.ds(i * q, q)], i, mate))
    last = send(part.at[mate], got.at[1], n_chunk, mate)
    hops = []
    for i in range(n_chunk):
        first[i].wait_recv()
        rows = pl.ds(i * q, q)
        pair[rows, :] = part[far, rows, :] + got[0, rows, :]
        if i > 0:
            rows = pl.ds((i - 1) * q, q)
            hops.append(send(pair.at[rows], far_got.at[rows], n_chunk + i, far))
    last.wait_recv()
    mine = part[ep] + got[1]
    rows = pl.ds((n_chunk - 1) * q, q)
    hops.append(send(pair.at[rows], far_got.at[rows], 2 * n_chunk, far))
    for i in range(n_chunk):
        hops[i].wait_recv()
        dx_ref[i * q:(i + 1) * q, :] = (mine[i * q:(i + 1) * q, :] + far_got[i * q:(i + 1) * q, :]).astype(BF16)
    for c in first + [last] + hops:
        c.wait_send()


def solution(mesh):
    n_src = mesh.shape['ep']
    vmem = pl.BlockSpec(memory_space=pltpu.VMEM)
    hbm = pl.BlockSpec(memory_space=pltpu.HBM)

    def local_step(x_loc, dy_loc, ids_loc, gate_loc, slot_loc, w_gate, w_down, w_up):
        tok, top_k = ids_loc.shape
        n_local, d_model, ff = w_gate.shape
        n_exp = n_local * n_src
        cap = slot_capacity(tok, top_k, n_exp)
        rows = n_src * cap
        n_tok = n_src * tok
        dma = pltpu.SemaphoreType.DMA
        xg, dyg, metag, w1, w3, w2 = pl.pallas_call(
            functools.partial(gather_kernel, cap),
            out_shape=(
                pltpu.VMEM((n_tok, d_model), BF16),
                pltpu.VMEM((n_tok, d_model), BF16),
                pltpu.VMEM((n_src, 16, 128), F32),
                pltpu.VMEM(w_gate.shape, BF16),
                pltpu.VMEM(w_up.shape, BF16),
                pltpu.VMEM(w_down.shape, BF16),
            ),
            in_specs=[hbm] * 8,
            out_specs=(vmem,) * 6,
            scratch_shapes=[
                pltpu.VMEM((tok, d_model), BF16),
                pltpu.VMEM((tok, d_model), BF16),
                pltpu.VMEM((top_k, tok), jnp.int32),
                pltpu.VMEM((top_k, tok), jnp.int32),
                pltpu.VMEM((top_k, tok), F32),
                pltpu.VMEM((16, 128), F32),
                dma((3, n_local)),
                dma((5,)),
                dma((15,)),
                dma((15,)),
            ],
            compiler_params=pltpu.CompilerParams(collective_id=0, has_side_effects=True, vmem_limit_bytes=4 << 20),
            name='gather',
        )(*(pltpu.with_memory_space_constraint(v, pltpu.HBM) for v in (x_loc, dy_loc, ids_loc.T, slot_loc.T, gate_loc.T, w_gate, w_up, w_down)))
        g1, g3, g2, part = pl.pallas_call(
            functools.partial(expert_kernel, cap, n_src),
            out_shape=(
                pltpu.HBM((n_local, d_model, ff), F32),
                pltpu.HBM((n_local, d_model, ff), F32),
                pltpu.HBM((n_local, ff, d_model), F32),
                pltpu.VMEM((n_src, tok, d_model), F32),
            ),
            in_specs=[vmem] * 6,
            out_specs=(hbm, hbm, hbm, vmem),
            scratch_shapes=[
                pltpu.VMEM((n_local, rows, n_tok), BF16),
                pltpu.VMEM((n_local, rows, d_model), BF16),
                pltpu.VMEM((n_local, rows, d_model), BF16),
                pltpu.VMEM((n_local, rows, d_model), BF16),
                pltpu.VMEM((2, d_model, ff), F32),
                pltpu.VMEM((2, d_model, ff), F32),
                pltpu.VMEM((2, ff, d_model), F32),
                dma((3, 2)),
            ],
            compiler_params=pltpu.CompilerParams(vmem_limit_bytes=24 << 20),
            name='experts',
        )(xg, dyg, metag, w1, w3, w2)
        dx_loc = pl.pallas_call(
            reduce_kernel,
            out_shape=jax.ShapeDtypeStruct((tok, d_model), BF16),
            in_specs=[vmem],
            out_specs=vmem,
            scratch_shapes=[
                pltpu.VMEM((2, tok, d_model), F32),
                pltpu.VMEM((tok, d_model), F32),
                pltpu.VMEM((tok, d_model), F32),
                dma((9,)),
                dma((9,)),
            ],
            compiler_params=pltpu.CompilerParams(collective_id=1, has_side_effects=True, vmem_limit_bytes=4 << 20),
            name='reduce',
        )(part)
        return dx_loc, g1, g2, g3

    tok_spec = P(('dp', 'ep'), None)
    w_spec = P('ep', None, None)
    grad_spec = P(('dp', 'ep'), None, None)
    return jax.shard_map(local_step, mesh=mesh, in_specs=(tok_spec, tok_spec, tok_spec, tok_spec, tok_spec, w_spec, w_spec, w_spec), out_specs=(tok_spec, grad_spec, grad_spec, grad_spec), check_vma=False)
```

```python
import functools

import jax
import jax.numpy as jnp
from jax import lax
from jax.experimental import pallas as pl
from jax.experimental.pallas import tpu as pltpu
from jax.sharding import PartitionSpec as P

MESH = pl.DeviceIdType.MESH
F32 = jnp.float32
BF16 = jnp.bfloat16
NN = (((1,), (0,)), ((), ()))
NT = (((1,), (1,)), ((), ()))
TN = (((0,), (0,)), ((), ()))
N_FIRST = 5
N_BUF = 4
N_EARLY = 5
N_MID = 4


def slot_capacity(tok_dev, top_k, n_exp):
    return ((3 * tok_dev * top_k) // (2 * n_exp) + 7) // 8 * 8


def mm(a, b, dims):
    return lax.dot_general(a, b, dims, preferred_element_type=F32)


def peers():
    ep = lax.axis_index('ep')
    core = lax.rem(ep, 2)
    chip = ep - core
    mate = chip + 1 - core
    far = lax.rem(ep + 2, 4)
    far_mate = lax.rem(mate + 2, 4)
    return ep, mate, far, far_mate


def entry_barrier(others):
    barrier = pltpu.get_barrier_semaphore()
    for other in others:
        pl.semaphore_signal(barrier, inc=1, device_id={'ep': other}, device_id_type=MESH)
    pl.semaphore_wait(barrier, len(others))


def run(lo, hi, body, unroll):
    def step(e, carry):
        body(e)
        return carry

    if unroll == 0:
        for e in range(lo, hi):
            body(e)
    else:
        lax.fori_loop(lo, hi, step, 0, unroll=unroll)


def gather_kernel(cap, x_hbm, dy_hbm, ids_hbm, slot_hbm, gate_hbm, w1_hbm, w3_hbm, w2_hbm, dyg, metag, p_all, x_all, a_all, b_all, w1t, w3t, w2t, xg, ids_ref, slot_ref, gate_ref, w1, w3, w2, w_sem, loc_sem, send_sem, recv_sem):
    ep, mate, far, far_mate = peers()
    n_local, rows, n_tok = p_all.shape
    n_src = metag.shape[0]
    tok = n_tok // n_src
    barrier = pltpu.get_barrier_semaphore()
    for other in (mate, far, far_mate):
        pl.semaphore_signal(barrier, inc=1, device_id={'ep': other}, device_id_type=MESH)
    mine = pl.multiple_of(ep * tok, tok)
    theirs = pl.multiple_of(far * tok, tok)
    small = []
    for k, (src, dst) in enumerate(((x_hbm, xg.at[pl.ds(mine, tok)]), (dy_hbm, dyg.at[pl.ds(mine, tok)]), (ids_hbm, ids_ref), (slot_hbm, slot_ref), (gate_hbm, gate_ref))):
        c = pltpu.make_async_copy(src, dst, loc_sem.at[k])
        c.start()
        small.append(c)

    def loads(e):
        return [pltpu.make_async_copy(src.at[e], dst.at[e], w_sem.at[k, e]) for k, (src, dst) in enumerate(((w1_hbm, w1), (w3_hbm, w3), (w2_hbm, w2)))]

    for e in range(n_local):
        for c in loads(e):
            c.start(priority=1)
    for c in small:
        c.wait()
    key = jnp.where(slot_ref[...] >= 0, ids_ref[...] * cap + slot_ref[...], -1)
    metag[ep, 0:8, 0:tok] = key.astype(F32)
    metag[ep, 8:16, 0:tok] = gate_ref[...]
    metag[ep, 0:8, tok:2 * tok] = jnp.zeros((8, tok), F32)
    metag[ep, 8:16, tok:2 * tok] = jnp.zeros((8, tok), F32)
    pl.semaphore_wait(barrier, 3)

    def send(src, dst, k, to):
        c = pltpu.make_async_remote_copy(src_ref=src, dst_ref=dst, send_sem=send_sem.at[k], recv_sem=recv_sem.at[k], device_id={'ep': to}, device_id_type=MESH)
        c.start()
        return c

    half = tok // 2
    pieces = [(ref, h * half) for ref in (xg, dyg) for h in range(2)]

    def block(ref, base, off):
        return ref.at[pl.ds(base + off, half)]

    to_far = [send(block(ref, mine, off), block(ref, mine, off), k, far) for k, (ref, off) in enumerate(pieces)]
    to_mate = [send(block(ref, mine, off), block(ref, mine, off), 4 + k, mate) for k, (ref, off) in enumerate(pieces)]
    metas = [send(metag.at[ep], metag.at[ep], 12 + k, to) for k, to in enumerate((far, mate, far_mate))]
    r256 = lax.broadcasted_iota(jnp.int32, (256, 256), 0)
    c256 = lax.broadcasted_iota(jnp.int32, (256, 256), 1)
    eye = jnp.where(r256 == c256, 1.0, 0.0).astype(BF16)

    def turn(e):
        for c in loads(e):
            c.wait()
        w1t[e] = w1[e].T
        w3t[e] = w3[e].T
        for q in range(w2.shape[2] // 256):
            w2t[e, q * 256:(q + 1) * 256, :] = mm(eye, w2[e, :, q * 256:(q + 1) * 256], NT).astype(BF16)

    relays = []

    def relay(k):
        ref, off = pieces[k]
        to_far[k].wait_recv()
        relays.append(send(block(ref, theirs, off), block(ref, theirs, off), 8 + k, mate))

    run(0, N_EARLY, turn, 1)
    relay(0)
    relay(1)
    run(N_EARLY, n_local, turn, 1)
    for c in to_mate[:2] + relays[:2] + metas:
        c.wait_recv()
    lane = lax.broadcasted_iota(jnp.int32, (1, n_tok), 1)
    src_base = (lane // tok) * cap
    row_id = lax.broadcasted_iota(jnp.int32, (rows, n_tok), 0)
    key = all_meta(metag, tok)[0:8, :].astype(jnp.int32)

    def front(e):
        lo = (ep * n_local + e) * cap
        hit = (key >= lo) & (key < lo + cap)
        slot = jnp.sum(jnp.where(hit, key - lo + 1, 0), axis=0, keepdims=True)
        want = jnp.where(slot > 0, slot - 1 + src_base, -1)
        sel = jnp.where(row_id == want, 1.0, 0.0).astype(BF16)
        p_all[e] = sel
        x_rows = mm(sel, xg[...], NN).astype(BF16)
        x_all[e] = x_rows
        a_all[e] = mm(x_rows, w1[e], NN).astype(BF16)
        b_all[e] = mm(x_rows, w3[e], NN).astype(BF16)

    run(0, N_MID, front, 2)
    relay(2)
    relay(3)
    run(N_MID, n_local, front, 2)
    for c in to_mate[2:] + relays[2:]:
        c.wait_recv()
    for c in to_far + to_mate + relays + metas:
        c.wait_send()


def all_meta(metag, tok):
    halves = []
    for pair in range(metag.shape[0] // 2):
        halves.append(metag[2 * pair] + pltpu.roll(metag[2 * pair + 1], tok, 1))
    return jnp.concatenate(halves, axis=1)


def grad_copies(stage, grads, out_sem, e, slot):
    return [pltpu.make_async_copy(s.at[slot], g.at[e], out_sem.at[k, slot]) for k, (s, g) in enumerate(zip(stage, grads))]


def weight_grads(rows_in, stage, e, slot):
    x_all, dz_all, h_all, da_all, db_all = rows_in
    s1, s3, s2 = stage
    x_rows = x_all[e]
    s2[slot] = mm(h_all[e], dz_all[e], TN)
    s1[slot] = mm(x_rows, da_all[e], TN)
    s3[slot] = mm(x_rows, db_all[e], TN)


def expert_kernel(cap, n_first, dyg, metag, p_all, x_all, a_all, b_all, w1t, w3t, w2t, g1, g3, g2, part, dz_all, h_all, da_all, db_all, dx_all, s1, s3, s2, out_sem):
    ep = lax.axis_index('ep')
    n_local, rows, n_tok = p_all.shape
    n_src = metag.shape[0]
    tok = n_tok // n_src
    meta = all_meta(metag, tok)
    key = meta[0:8, :].astype(jnp.int32)
    gate = meta[8:16, :]
    rows_in = (x_all, dz_all, h_all, da_all, db_all)
    stage = (s1, s3, s2)
    grads = (g1, g3, g2)

    def middle(e):
        lo = (ep * n_local + e) * cap
        g_tok = jnp.sum(jnp.where((key >= lo) & (key < lo + cap), gate, 0.0), axis=0, keepdims=True)
        sel = p_all[e]
        g_row = jnp.sum(sel.astype(F32) * g_tok, axis=1, keepdims=True)
        dz_rows = (g_row * mm(sel, dyg[...], NN)).astype(BF16)
        dz_all[e] = dz_rows
        dh = mm(dz_rows, w2t[e], NN)
        a = a_all[e].astype(F32)
        b = b_all[e].astype(F32)
        sg = jax.nn.sigmoid(a)
        silu = a * sg
        h_all[e] = (silu * b).astype(BF16)
        da_all[e] = (dh * b * sg * (1.0 + a * (1.0 - sg))).astype(BF16)
        db_all[e] = (dh * silu).astype(BF16)

    def back(e):
        dx_all[e] = (mm(da_all[e], w1t[e], NN) + mm(db_all[e], w3t[e], NN)).astype(BF16)

    def first(e):
        middle(e)
        back(e)
        slot = lax.rem(e, 2)

        @pl.when(e >= 2)
        def _():
            for c in grad_copies(stage, grads, out_sem, e - 2, slot):
                c.wait()

        weight_grads(rows_in, stage, e, slot)
        for c in grad_copies(stage, grads, out_sem, e, slot):
            c.start()

    def later(e):
        middle(e)
        back(e)

    run(0, n_first, first, 1)
    run(n_first, n_local, later, 1)
    total = mm(p_all[...].reshape(n_local * rows, n_tok), dx_all[...].reshape(n_local * rows, -1), TN)
    for s in range(n_src):
        part[s] = total[s * tok:(s + 1) * tok]
    for e in range(max(n_first - 2, 0), n_first):
        for c in grad_copies(stage, grads, out_sem, e, e % 2):
            c.wait()


def rest_kernel(n_first, x_all, dz_all, h_all, da_all, db_all, g1_in, g3_in, g2_in, g1, g3, g2, s1, s3, s2, out_sem):
    del g1_in, g3_in, g2_in
    n_local = x_all.shape[0]
    n_buf = s1.shape[0]
    stage = (s1, s3, s2)
    grads = (g1, g3, g2)
    for e in range(n_first, n_local):
        slot = (e - n_first) % n_buf
        if e - n_first >= n_buf:
            for c in grad_copies(stage, grads, out_sem, e - n_buf, slot):
                c.wait()
        weight_grads((x_all, dz_all, h_all, da_all, db_all), stage, e, slot)
        for c in grad_copies(stage, grads, out_sem, e, slot):
            c.start()
    for e in range(max(n_first, n_local - n_buf), n_local):
        for c in grad_copies(stage, grads, out_sem, e, (e - n_first) % n_buf):
            c.wait()


def pair_kernel(part, mine_ref, theirs_ref, got, send_sem, recv_sem):
    ep, mate, far, far_mate = peers()
    entry_barrier((mate,))
    sends = []
    for k, owner in enumerate((far_mate, mate)):
        c = pltpu.make_async_remote_copy(src_ref=part.at[owner], dst_ref=got.at[k], send_sem=send_sem.at[k], recv_sem=recv_sem.at[k], device_id={'ep': mate}, device_id_type=MESH)
        c.start()
        sends.append(c)
    sends[0].wait_recv()
    theirs_ref[...] = part[far] + got[0]
    sends[1].wait_recv()
    mine_ref[...] = part[ep] + got[1]
    for c in sends:
        c.wait_send()


def solution(mesh):
    n_src = mesh.shape['ep']
    vmem = pl.BlockSpec(memory_space=pltpu.VMEM)
    hbm = pl.BlockSpec(memory_space=pltpu.HBM)

    def local_step(x_loc, dy_loc, ids_loc, gate_loc, slot_loc, w_gate, w_down, w_up):
        tok, top_k = ids_loc.shape
        n_local, d_model, ff = w_gate.shape
        n_exp = n_local * n_src
        cap = slot_capacity(tok, top_k, n_exp)
        rows = n_src * cap
        n_tok = n_src * tok
        dma = pltpu.SemaphoreType.DMA
        fixed = lambda v: pltpu.with_memory_space_constraint(v, pltpu.HBM)
        turned = tuple(pltpu.VMEM((n_local, w.shape[2], w.shape[1]), BF16) for w in (w_gate, w_up, w_down))
        dyg, metag, p_all, x_all, a_all, b_all, w1t, w3t, w2t = pl.pallas_call(
            functools.partial(gather_kernel, cap),
            out_shape=(
                pltpu.VMEM((n_tok, d_model), BF16),
                pltpu.VMEM((n_src, 16, 128), F32),
                pltpu.VMEM((n_local, rows, n_tok), BF16),
                pltpu.VMEM((n_local, rows, d_model), BF16),
                pltpu.VMEM((n_local, rows, ff), BF16),
                pltpu.VMEM((n_local, rows, ff), BF16),
            ) + turned,
            in_specs=[hbm] * 8,
            out_specs=(vmem,) * 9,
            scratch_shapes=[
                pltpu.VMEM((n_tok, d_model), BF16),
                pltpu.VMEM((top_k, tok), jnp.int32),
                pltpu.VMEM((top_k, tok), jnp.int32),
                pltpu.VMEM((top_k, tok), F32),
                *(pltpu.VMEM(w.shape, BF16) for w in (w_gate, w_up, w_down)),
                dma((3, n_local)),
                dma((5,)),
                dma((15,)),
                dma((15,)),
            ],
            compiler_params=pltpu.CompilerParams(collective_id=0, has_side_effects=True, vmem_limit_bytes=27 << 20),
            name='gather',
        )(*map(fixed, (x_loc, dy_loc, ids_loc.T, slot_loc.T, gate_loc.T, w_gate, w_up, w_down)))
        grad_shapes = tuple(pltpu.HBM(w.shape, F32) for w in (w_gate, w_up, w_down))
        stage = lambda n: [pltpu.VMEM((n,) + w.shape[1:], F32) for w in (w_gate, w_up, w_down)]
        row_bytes = n_local * rows * (2 * d_model + 3 * ff) * 2
        g1, g3, g2, part, dz_all, h_all, da_all, db_all = pl.pallas_call(
            functools.partial(expert_kernel, cap, N_FIRST),
            out_shape=grad_shapes + (
                pltpu.VMEM((n_src, tok, d_model), F32),
                pltpu.VMEM((n_local, rows, d_model), BF16),
                pltpu.VMEM((n_local, rows, ff), BF16),
                pltpu.VMEM((n_local, rows, ff), BF16),
                pltpu.VMEM((n_local, rows, ff), BF16),
            ),
            in_specs=[vmem] * 9,
            out_specs=(hbm,) * 3 + (vmem,) * 5,
            scratch_shapes=[pltpu.VMEM((n_local, rows, d_model), BF16), *stage(2), dma((3, 2))],
            compiler_params=pltpu.CompilerParams(vmem_limit_bytes=20 << 20),
            name='experts',
        )(dyg, metag, p_all, x_all, a_all, b_all, w1t, w3t, w2t)
        rows_in = (x_all, dz_all, h_all, da_all, db_all)
        mine, theirs = pl.pallas_call(
            pair_kernel,
            out_shape=(pltpu.VMEM((tok, d_model), F32),) * 2,
            in_specs=[vmem],
            out_specs=(vmem,) * 2,
            scratch_shapes=[pltpu.VMEM((2, tok, d_model), F32), dma((2,)), dma((2,))],
            compiler_params=pltpu.CompilerParams(collective_id=1, has_side_effects=True, vmem_limit_bytes=4 << 20),
            name='pair',
        )(part)
        far = lax.ppermute(theirs, 'ep', [(i, (i + 2) % n_src) for i in range(n_src)])
        n_rest = n_local - N_FIRST
        g1, g3, g2 = pl.pallas_call(
            functools.partial(rest_kernel, N_FIRST),
            out_shape=grad_shapes,
            in_specs=[vmem] * 5 + [hbm] * 3,
            out_specs=(hbm,) * 3,
            scratch_shapes=[*stage(N_BUF), dma((3, N_BUF))],
            input_output_aliases={5: 0, 6: 1, 7: 2},
            compiler_params=pltpu.CompilerParams(vmem_limit_bytes=40 << 20),
            cost_estimate=pl.CostEstimate(flops=2 * 3 * n_rest * rows * d_model * ff, bytes_accessed=n_rest * 3 * d_model * ff * 4 + row_bytes, transcendentals=0),
            name='rest',
        )(*rows_in, g1, g3, g2)
        dx_loc = (mine + far).astype(BF16)
        return dx_loc, g1, g2, g3

    tok_spec = P(('dp', 'ep'), None)
    w_spec = P('ep', None, None)
    grad_spec = P(('dp', 'ep'), None, None)
    return jax.shard_map(local_step, mesh=mesh, in_specs=(tok_spec, tok_spec, tok_spec, tok_spec, tok_spec, w_spec, w_spec, w_spec), out_specs=(tok_spec, grad_spec, grad_spec, grad_spec), check_vma=False)
```

```python
import functools

import jax
import jax.numpy as jnp
from jax import lax
from jax.experimental import pallas as pl
from jax.experimental.pallas import tpu as pltpu
from jax.sharding import PartitionSpec as P

MESH = pl.DeviceIdType.MESH
F32 = jnp.float32
BF16 = jnp.bfloat16
NN = (((1,), (0,)), ((), ()))
NT = (((1,), (1,)), ((), ()))
TN = (((0,), (0,)), ((), ()))
N_FIRST = 5
N_BUF = 3
N_RING = 6
U_ROUTE = 2
U_PAIR = 4
STEPS = (0, 1, 3, 4, 6)


def slot_capacity(tok_dev, top_k, n_exp):
    return ((3 * tok_dev * top_k) // (2 * n_exp) + 7) // 8 * 8


def mm(a, b, dims):
    return lax.dot_general(a, b, dims, preferred_element_type=F32)


def peers():
    ep = lax.axis_index('ep')
    core = lax.rem(ep, 2)
    chip = ep - core
    mate = chip + 1 - core
    far = lax.rem(ep + 2, 4)
    far_mate = lax.rem(mate + 2, 4)
    return ep, mate, far, far_mate


def entry_barrier(others):
    barrier = pltpu.get_barrier_semaphore()
    for other in others:
        pl.semaphore_signal(barrier, inc=1, device_id={'ep': other}, device_id_type=MESH)
    pl.semaphore_wait(barrier, len(others))


def run(lo, hi, body, unroll):
    def step(e, carry):
        body(e)
        return carry

    if unroll == 0:
        for e in range(lo, hi):
            body(e)
    else:
        lax.fori_loop(lo, hi, step, 0, unroll=unroll)


def gather_kernel(cap, x_hbm, dy_hbm, ids_hbm, slot_hbm, gate_hbm, w1_hbm, w3_hbm, w2_hbm, p_all, x_all, dz_all, a_all, b_all, w1t, w3t, w2t, xg, dyg, metag, g_rows, ids_ref, slot_ref, gate_ref, w1, w3, w2, w_sem, loc_sem, send_sem, recv_sem):
    ep, mate, far, far_mate = peers()
    n_local, rows, n_tok = p_all.shape
    n_src = metag.shape[0]
    tok = n_tok // n_src
    barrier = pltpu.get_barrier_semaphore()
    for other in (mate, far, far_mate):
        pl.semaphore_signal(barrier, inc=1, device_id={'ep': other}, device_id_type=MESH)
    mine = pl.multiple_of(ep * tok, tok)
    theirs = pl.multiple_of(far * tok, tok)
    small = []
    for k, (src, dst) in enumerate(((x_hbm, xg.at[pl.ds(mine, tok)]), (dy_hbm, dyg.at[pl.ds(mine, tok)]), (ids_hbm, ids_ref), (slot_hbm, slot_ref), (gate_hbm, gate_ref))):
        c = pltpu.make_async_copy(src, dst, loc_sem.at[k])
        c.start()
        small.append(c)

    n_ring = w2.shape[0]

    def load_w2(e):
        return pltpu.make_async_copy(w2_hbm.at[e], w2.at[lax.rem(e, n_ring)], w_sem.at[2, e])

    def loads(e):
        return [pltpu.make_async_copy(src.at[e], dst.at[e], w_sem.at[k, e]) for k, (src, dst) in enumerate(((w1_hbm, w1), (w3_hbm, w3)))]

    for e in range(n_local):
        for c in loads(e):
            c.start(priority=1)
        if e < n_ring:
            load_w2(e).start(priority=1)
    for c in small:
        c.wait()
    key = jnp.where(slot_ref[...] >= 0, ids_ref[...] * cap + slot_ref[...], -1)
    metag[ep, 0:8, 0:tok] = key.astype(F32)
    metag[ep, 8:16, 0:tok] = gate_ref[...]
    metag[ep, 0:8, tok:2 * tok] = jnp.zeros((8, tok), F32)
    metag[ep, 8:16, tok:2 * tok] = jnp.zeros((8, tok), F32)
    pl.semaphore_wait(barrier, 3)

    def send(src, dst, k, to):
        c = pltpu.make_async_remote_copy(src_ref=src, dst_ref=dst, send_sem=send_sem.at[k], recv_sem=recv_sem.at[k], device_id={'ep': to}, device_id_type=MESH)
        c.start()
        return c

    half = tok // 2
    pieces = [(ref, h * half) for ref in (xg, dyg) for h in range(2)]

    def block(ref, base, off):
        return ref.at[pl.ds(base + off, half)]

    metas = [send(metag.at[ep], metag.at[ep], 12 + k, to) for k, to in enumerate((far, mate, far_mate))]
    to_far = [send(block(ref, mine, off), block(ref, mine, off), k, far) for k, (ref, off) in enumerate(pieces)]
    to_mate = [send(block(ref, mine, off), block(ref, mine, off), 4 + k, mate) for k, (ref, off) in enumerate(pieces)]
    r256 = lax.broadcasted_iota(jnp.int32, (256, 256), 0)
    c256 = lax.broadcasted_iota(jnp.int32, (256, 256), 1)
    eye = jnp.where(r256 == c256, 1.0, 0.0).astype(BF16)

    def turn(e):
        for c in loads(e):
            c.wait()
        load_w2(e).wait()
        w1t[e] = w1[e].T
        w3t[e] = w3[e].T
        slot = lax.rem(e, n_ring)
        for q in range(w2.shape[2] // 256):
            w2t[e, q * 256:(q + 1) * 256, :] = mm(eye, w2[slot, :, q * 256:(q + 1) * 256], NT).astype(BF16)

    relays = []

    def relay(k):
        ref, off = pieces[k]
        to_far[k].wait_recv()
        relays.append(send(block(ref, theirs, off), block(ref, theirs, off), 8 + k, mate))

    def turn_load(e):
        turn(e)
        load_w2(e + n_ring).start(priority=1)

    run(0, n_local - n_ring, turn_load, 1)
    run(n_local - n_ring, 4, turn, 1)
    for c in metas:
        c.wait_recv()
    lane = lax.broadcasted_iota(jnp.int32, (1, n_tok), 1)
    src_base = (lane // tok) * cap
    row_id = lax.broadcasted_iota(jnp.int32, (rows, n_tok), 0)
    meta = all_meta(metag, tok)
    key = meta[0:8, :].astype(jnp.int32)
    gate = meta[8:16, :]

    def route(e):
        lo = (ep * n_local + e) * cap
        hit = (key >= lo) & (key < lo + cap)
        slot = jnp.sum(jnp.where(hit, key - lo + 1, 0), axis=0, keepdims=True)
        g_tok = jnp.sum(jnp.where(hit, gate, 0.0), axis=0, keepdims=True)
        pick = row_id == jnp.where(slot > 0, slot - 1 + src_base, -1)
        p_all[e] = jnp.where(pick, 1.0, 0.0).astype(BF16)
        g_rows[e] = jnp.broadcast_to(jnp.sum(jnp.where(pick, g_tok, 0.0), axis=1, keepdims=True), g_rows.shape[1:])

    run(0, n_local, route, U_ROUTE)
    turn(4)
    relay(0)
    relay(1)
    turn(5)
    for c in to_mate[:2] + relays[:2]:
        c.wait_recv()

    def spread(i):
        two = pl.ds(i * 2, 2)
        x_all[two] = mm(p_all[two].reshape(2 * rows, n_tok), xg[...], NN).astype(BF16).reshape(2, rows, -1)

    def front(e):
        a_all[e] = mm(x_all[e], w1[e], NN).astype(BF16)
        b_all[e] = mm(x_all[e], w3[e], NN).astype(BF16)

    run(0, n_local // 2, spread, U_PAIR)
    front(0)
    turn(6)
    front(1)
    front(2)
    relay(2)
    relay(3)
    front(3)
    turn(7)
    for e in range(4, n_local):
        front(e)
    for c in to_mate[2:] + relays[2:]:
        c.wait_recv()

    def scale(i):
        two = pl.ds(i * 2, 2)
        dy_rows = mm(p_all[two].reshape(2 * rows, n_tok), dyg[...], NN).reshape(2, rows, -1)
        dz_all[two] = (g_rows[two][:, :, 0:1] * dy_rows).astype(BF16)

    run(0, n_local // 2, scale, U_PAIR)
    for c in to_far + to_mate + relays + metas:
        c.wait_send()


def all_meta(metag, tok):
    halves = []
    for pair in range(metag.shape[0] // 2):
        halves.append(metag[2 * pair] + pltpu.roll(metag[2 * pair + 1], tok, 1))
    return jnp.concatenate(halves, axis=1)


def grad_copies(stage, grads, out_sem, e, slot):
    return [pltpu.make_async_copy(s.at[slot], g.at[e], out_sem.at[k, slot]) for k, (s, g) in enumerate(zip(stage, grads))]


def weight_grads(rows_in, stage, e, slot):
    x_all, dz_all, h_all, da_all, db_all = rows_in
    s1, s3, s2 = stage
    x_rows = x_all[e]
    s2[slot] = mm(h_all[e], dz_all[e], TN)
    s1[slot] = mm(x_rows, da_all[e], TN)
    s3[slot] = mm(x_rows, db_all[e], TN)


def expert_kernel(n_first, p_all, x_all, dz_all, a_all, b_all, w1t, w3t, w2t, g1, g3, g2, part, h_all, da_all, db_all, dx_all, s1, s3, s2, out_sem):
    n_local, rows, n_tok = p_all.shape
    n_src, tok, _ = part.shape
    rows_in = (x_all, dz_all, h_all, da_all, db_all)
    stage = (s1, s3, s2)
    grads = (g1, g3, g2)

    def middle(e):
        dh = mm(dz_all[e], w2t[e], NN)
        a = a_all[e].astype(F32)
        b = b_all[e].astype(F32)
        sg = jax.nn.sigmoid(a)
        silu = a * sg
        h_all[e] = (silu * b).astype(BF16)
        da_all[e] = (dh * b * sg * (1.0 + a * (1.0 - sg))).astype(BF16)
        db_all[e] = (dh * silu).astype(BF16)

    def back(e):
        dx_all[e] = (mm(da_all[e], w1t[e], NN) + mm(db_all[e], w3t[e], NN)).astype(BF16)

    def grads_of(e):
        if e >= 2:
            for c in grad_copies(stage, grads, out_sem, e - 2, e % 2):
                c.wait()
        weight_grads(rows_in, stage, e, e % 2)
        for c in grad_copies(stage, grads, out_sem, e, e % 2):
            c.start()

    middle(0)
    for e in range(n_local):
        if e + 1 < n_local:
            middle(e + 1)
        if e in STEPS:
            grads_of(STEPS.index(e))
        back(e)
    total = mm(p_all[...].reshape(n_local * rows, n_tok), dx_all[...].reshape(n_local * rows, -1), TN)
    for s in range(n_src):
        part[s] = total[s * tok:(s + 1) * tok]
    for e in range(max(n_first - 2, 0), n_first):
        for c in grad_copies(stage, grads, out_sem, e, e % 2):
            c.wait()


def rest_kernel(n_first, x_all, dz_all, h_all, da_all, db_all, g1_in, g3_in, g2_in, g1, g3, g2, s1, s3, s2, out_sem):
    del g1_in, g3_in, g2_in
    n_local = x_all.shape[0]
    n_buf = s1.shape[0]
    stage = (s1, s3, s2)
    grads = (g1, g3, g2)
    for e in range(n_first, n_local):
        slot = (e - n_first) % n_buf
        if e - n_first >= n_buf:
            for c in grad_copies(stage, grads, out_sem, e - n_buf, slot):
                c.wait()
        weight_grads((x_all, dz_all, h_all, da_all, db_all), stage, e, slot)
        for c in grad_copies(stage, grads, out_sem, e, slot):
            c.start()
    for e in range(max(n_first, n_local - n_buf), n_local):
        for c in grad_copies(stage, grads, out_sem, e, (e - n_first) % n_buf):
            c.wait()


def pair_kernel(part, mine_ref, theirs_ref, got, send_sem, recv_sem):
    ep, mate, far, far_mate = peers()
    entry_barrier((mate,))
    sends = []
    for k, owner in enumerate((far_mate, mate)):
        c = pltpu.make_async_remote_copy(src_ref=part.at[owner], dst_ref=got.at[k], send_sem=send_sem.at[k], recv_sem=recv_sem.at[k], device_id={'ep': mate}, device_id_type=MESH)
        c.start()
        sends.append(c)
    sends[0].wait_recv()
    theirs_ref[...] = part[far] + got[0]
    sends[1].wait_recv()
    mine_ref[...] = part[ep] + got[1]
    for c in sends:
        c.wait_send()


def solution(mesh):
    n_src = mesh.shape['ep']
    vmem = pl.BlockSpec(memory_space=pltpu.VMEM)
    hbm = pl.BlockSpec(memory_space=pltpu.HBM)

    def local_step(x_loc, dy_loc, ids_loc, gate_loc, slot_loc, w_gate, w_down, w_up):
        tok, top_k = ids_loc.shape
        n_local, d_model, ff = w_gate.shape
        n_exp = n_local * n_src
        cap = slot_capacity(tok, top_k, n_exp)
        rows = n_src * cap
        n_tok = n_src * tok
        dma = pltpu.SemaphoreType.DMA
        fixed = lambda v: pltpu.with_memory_space_constraint(v, pltpu.HBM)
        turned = tuple(pltpu.VMEM((n_local, w.shape[2], w.shape[1]), BF16) for w in (w_gate, w_up, w_down))
        p_all, x_all, dz_all, a_all, b_all, w1t, w3t, w2t = pl.pallas_call(
            functools.partial(gather_kernel, cap),
            out_shape=(
                pltpu.VMEM((n_local, rows, n_tok), BF16),
                pltpu.VMEM((n_local, rows, d_model), BF16),
                pltpu.VMEM((n_local, rows, d_model), BF16),
                pltpu.VMEM((n_local, rows, ff), BF16),
                pltpu.VMEM((n_local, rows, ff), BF16),
            ) + turned,
            in_specs=[hbm] * 8,
            out_specs=(vmem,) * 8,
            scratch_shapes=[
                pltpu.VMEM((n_tok, d_model), BF16),
                pltpu.VMEM((n_tok, d_model), BF16),
                pltpu.VMEM((n_src, 16, 128), F32),
                pltpu.VMEM((n_local, rows, 128), F32),
                pltpu.VMEM((top_k, tok), jnp.int32),
                pltpu.VMEM((top_k, tok), jnp.int32),
                pltpu.VMEM((top_k, tok), F32),
                pltpu.VMEM(w_gate.shape, BF16),
                pltpu.VMEM(w_up.shape, BF16),
                pltpu.VMEM((N_RING,) + w_down.shape[1:], BF16),
                dma((3, n_local)),
                dma((5,)),
                dma((15,)),
                dma((15,)),
            ],
            compiler_params=pltpu.CompilerParams(collective_id=0, has_side_effects=True, vmem_limit_bytes=24 << 20),
            name='gather',
        )(*map(fixed, (x_loc, dy_loc, ids_loc.T, slot_loc.T, gate_loc.T, w_gate, w_up, w_down)))
        grad_shapes = tuple(pltpu.HBM(w.shape, F32) for w in (w_gate, w_up, w_down))
        stage = lambda n: [pltpu.VMEM((n,) + w.shape[1:], F32) for w in (w_gate, w_up, w_down)]
        row_bytes = n_local * rows * (2 * d_model + 3 * ff) * 2
        g1, g3, g2, part, h_all, da_all, db_all = pl.pallas_call(
            functools.partial(expert_kernel, N_FIRST),
            out_shape=grad_shapes + (
                pltpu.VMEM((n_src, tok, d_model), F32),
                pltpu.VMEM((n_local, rows, ff), BF16),
                pltpu.VMEM((n_local, rows, ff), BF16),
                pltpu.VMEM((n_local, rows, ff), BF16),
            ),
            in_specs=[vmem] * 8,
            out_specs=(hbm,) * 3 + (vmem,) * 4,
            scratch_shapes=[pltpu.VMEM((n_local, rows, d_model), BF16), *stage(2), dma((3, 2))],
            compiler_params=pltpu.CompilerParams(vmem_limit_bytes=20 << 20),
            name='experts',
        )(p_all, x_all, dz_all, a_all, b_all, w1t, w3t, w2t)
        rows_in = (x_all, dz_all, h_all, da_all, db_all)
        mine, theirs = pl.pallas_call(
            pair_kernel,
            out_shape=(pltpu.VMEM((tok, d_model), F32),) * 2,
            in_specs=[vmem],
            out_specs=(vmem,) * 2,
            scratch_shapes=[pltpu.VMEM((2, tok, d_model), F32), dma((2,)), dma((2,))],
            compiler_params=pltpu.CompilerParams(collective_id=1, has_side_effects=True, vmem_limit_bytes=4 << 20),
            name='pair',
        )(part)
        far = lax.ppermute(theirs, 'ep', [(i, (i + 2) % n_src) for i in range(n_src)])
        n_rest = n_local - N_FIRST
        g1, g3, g2 = pl.pallas_call(
            functools.partial(rest_kernel, N_FIRST),
            out_shape=grad_shapes,
            in_specs=[vmem] * 5 + [hbm] * 3,
            out_specs=(hbm,) * 3,
            scratch_shapes=[*stage(N_BUF), dma((3, N_BUF))],
            input_output_aliases={5: 0, 6: 1, 7: 2},
            compiler_params=pltpu.CompilerParams(vmem_limit_bytes=20 << 20),
            cost_estimate=pl.CostEstimate(flops=2 * 3 * n_rest * rows * d_model * ff, bytes_accessed=n_rest * 3 * d_model * ff * 4 + row_bytes, transcendentals=0),
            name='rest',
        )(*rows_in, g1, g3, g2)
        dx_loc = (mine + far).astype(BF16)
        return dx_loc, g1, g2, g3

    tok_spec = P(('dp', 'ep'), None)
    w_spec = P('ep', None, None)
    grad_spec = P(('dp', 'ep'), None, None)
    return jax.shard_map(local_step, mesh=mesh, in_specs=(tok_spec, tok_spec, tok_spec, tok_spec, tok_spec, w_spec, w_spec, w_spec), out_specs=(tok_spec, grad_spec, grad_spec, grad_spec), check_vma=False)
```

```python
import functools

import jax
import jax.numpy as jnp
from jax import lax
from jax.experimental import pallas as pl
from jax.experimental.pallas import tpu as pltpu
from jax.sharding import PartitionSpec as P

MESH = pl.DeviceIdType.MESH
F32 = jnp.float32
BF16 = jnp.bfloat16
NN = (((1,), (0,)), ((), ()))
NT = (((1,), (1,)), ((), ()))
TN = (((0,), (0,)), ((), ()))
N_FIRST = 5
N_BUF = 3
N_STAGE = 2
N_RING = 6
U_ROUTE = 2
U_PAIR = 4
STEPS = (0, 1, 2, 4, 5)


def slot_capacity(tok_dev, top_k, n_exp):
    return ((3 * tok_dev * top_k) // (2 * n_exp) + 7) // 8 * 8


def mm(a, b, dims):
    return lax.dot_general(a, b, dims, preferred_element_type=F32)


def peers():
    ep = lax.axis_index('ep')
    core = lax.rem(ep, 2)
    chip = ep - core
    mate = chip + 1 - core
    far = lax.rem(ep + 2, 4)
    far_mate = lax.rem(mate + 2, 4)
    return ep, mate, far, far_mate


def entry_barrier(others):
    barrier = pltpu.get_barrier_semaphore()
    for other in others:
        pl.semaphore_signal(barrier, inc=1, device_id={'ep': other}, device_id_type=MESH)
    pl.semaphore_wait(barrier, len(others))


def run(lo, hi, body, unroll):
    def step(e, carry):
        body(e)
        return carry

    if unroll == 0:
        for e in range(lo, hi):
            body(e)
    else:
        lax.fori_loop(lo, hi, step, 0, unroll=unroll)


def gather_kernel(cap, x_hbm, dy_hbm, ids_hbm, slot_hbm, gate_hbm, w1_hbm, w3_hbm, w2_hbm, p_all, x_all, dz_all, a_all, b_all, w1t, w3t, w2t, xg, dyg, metag, g_rows, ids_ref, slot_ref, gate_ref, w1, w3, w2, w_sem, loc_sem, send_sem, recv_sem):
    ep, mate, far, far_mate = peers()
    n_local, rows, n_tok = p_all.shape
    n_src = metag.shape[0]
    tok = n_tok // n_src
    barrier = pltpu.get_barrier_semaphore()
    for other in (mate, far, far_mate):
        pl.semaphore_signal(barrier, inc=1, device_id={'ep': other}, device_id_type=MESH)
    mine = pl.multiple_of(ep * tok, tok)
    theirs = pl.multiple_of(far * tok, tok)
    small = []
    for k, (src, dst) in enumerate(((x_hbm, xg.at[pl.ds(mine, tok)]), (dy_hbm, dyg.at[pl.ds(mine, tok)]), (ids_hbm, ids_ref), (slot_hbm, slot_ref), (gate_hbm, gate_ref))):
        c = pltpu.make_async_copy(src, dst, loc_sem.at[k])
        c.start()
        small.append(c)

    n_ring = w2.shape[0]

    def load_w2(e):
        return pltpu.make_async_copy(w2_hbm.at[e], w2.at[lax.rem(e, n_ring)], w_sem.at[2, e])

    def loads(e):
        return [pltpu.make_async_copy(src.at[e], dst.at[e], w_sem.at[k, e]) for k, (src, dst) in enumerate(((w1_hbm, w1), (w3_hbm, w3)))]

    for e in range(n_local):
        for c in loads(e):
            c.start(priority=1)
        if e < n_ring:
            load_w2(e).start(priority=1)
    for c in small:
        c.wait()
    key = jnp.where(slot_ref[...] >= 0, ids_ref[...] * cap + slot_ref[...], -1)
    metag[ep, 0:8, 0:tok] = key.astype(F32)
    metag[ep, 8:16, 0:tok] = gate_ref[...]
    metag[ep, 0:8, tok:2 * tok] = jnp.zeros((8, tok), F32)
    metag[ep, 8:16, tok:2 * tok] = jnp.zeros((8, tok), F32)
    pl.semaphore_wait(barrier, 3)

    def send(src, dst, k, to):
        c = pltpu.make_async_remote_copy(src_ref=src, dst_ref=dst, send_sem=send_sem.at[k], recv_sem=recv_sem.at[k], device_id={'ep': to}, device_id_type=MESH)
        c.start()
        return c

    half = tok // 2
    pieces = [(ref, h * half) for ref in (xg, dyg) for h in range(2)]

    def block(ref, base, off):
        return ref.at[pl.ds(base + off, half)]

    metas = [send(metag.at[ep], metag.at[ep], 12 + k, to) for k, to in enumerate((far, mate, far_mate))]
    to_far = [send(block(ref, mine, off), block(ref, mine, off), k, far) for k, (ref, off) in enumerate(pieces)]
    to_mate = [send(block(ref, mine, off), block(ref, mine, off), 4 + k, mate) for k, (ref, off) in enumerate(pieces)]
    r256 = lax.broadcasted_iota(jnp.int32, (256, 256), 0)
    c256 = lax.broadcasted_iota(jnp.int32, (256, 256), 1)
    eye = jnp.where(r256 == c256, 1.0, 0.0).astype(BF16)

    def ready(e):
        for c in loads(e):
            c.wait()
        load_w2(e).wait()

    def flip(e):
        w1t[e] = w1[e].T
        w3t[e] = w3[e].T
        slot = lax.rem(e, n_ring)
        w2t[e] = w2[slot].T

    def turn(e):
        ready(e)
        flip(e)

    relays = []

    def relay(k):
        ref, off = pieces[k]
        to_far[k].wait_recv()
        relays.append(send(block(ref, theirs, off), block(ref, theirs, off), 8 + k, mate))

    def turn_load(e):
        turn(e)
        load_w2(e + n_ring).start(priority=1)

    run(0, n_local - n_ring, turn_load, 1)
    run(n_local - n_ring, 4, turn, 1)
    for c in metas:
        c.wait_recv()
    lane = lax.broadcasted_iota(jnp.int32, (1, n_tok), 1)
    src_base = (lane // tok) * cap
    row_id = lax.broadcasted_iota(jnp.int32, (rows, n_tok), 0)
    meta = all_meta(metag, tok)
    key = meta[0:8, :].astype(jnp.int32)
    gate = meta[8:16, :]

    def route(e):
        lo = (ep * n_local + e) * cap
        hit = (key >= lo) & (key < lo + cap)
        slot = jnp.sum(jnp.where(hit, key - lo + 1, 0), axis=0, keepdims=True)
        g_tok = jnp.sum(jnp.where(hit, gate, 0.0), axis=0, keepdims=True)
        pick = row_id == jnp.where(slot > 0, slot - 1 + src_base, -1)
        p_all[e] = jnp.where(pick, 1.0, 0.0).astype(BF16)
        g_rows[e] = jnp.broadcast_to(jnp.sum(jnp.where(pick, g_tok, 0.0), axis=1, keepdims=True), g_rows.shape[1:])

    run(0, n_local, route, U_ROUTE)
    turn(4)
    relay(0)
    relay(1)
    turn(5)
    for c in to_mate[:2] + relays[:2]:
        c.wait_recv()

    def spread(i):
        two = pl.ds(i * 2, 2)
        x_all[two] = mm(p_all[two].reshape(2 * rows, n_tok), xg[...], NN).astype(BF16).reshape(2, rows, -1)

    def front(e):
        a_all[e] = mm(x_all[e], w1[e], NN).astype(BF16)
        b_all[e] = mm(x_all[e], w3[e], NN).astype(BF16)

    ready(6)
    for i in range(n_local // 2):
        spread(i)
    front(0)
    flip(6)
    front(1)
    relay(2)
    relay(3)
    ready(7)
    front(2)
    flip(7)
    for e in range(3, n_local):
        front(e)
    for c in to_mate[2:] + relays[2:]:
        c.wait_recv()

    def scale(i):
        two = pl.ds(i * 2, 2)
        dy_rows = mm(p_all[two].reshape(2 * rows, n_tok), dyg[...], NN).reshape(2, rows, -1)
        dz_all[two] = (g_rows[two][:, :, 0:1] * dy_rows).astype(BF16)

    run(0, n_local // 2, scale, U_PAIR)
    for c in to_far + to_mate + relays + metas:
        c.wait_send()


def all_meta(metag, tok):
    halves = []
    for pair in range(metag.shape[0] // 2):
        halves.append(metag[2 * pair] + pltpu.roll(metag[2 * pair + 1], tok, 1))
    return jnp.concatenate(halves, axis=1)


def grad_copy(stage, grads, out_sem, k, e, slot):
    return pltpu.make_async_copy(stage[k].at[slot], grads[k].at[e], out_sem.at[k, slot])


def weight_grad(rows_in, stage, grads, out_sem, k, e, slot, prev):
    x_all, dz_all, h_all, da_all, db_all = rows_in
    if prev >= 0:
        grad_copy(stage, grads, out_sem, k, prev, slot).wait()
    left, right = ((x_all, da_all), (x_all, db_all), (h_all, dz_all))[k]
    stage[k][slot] = mm(left[e], right[e], TN)
    grad_copy(stage, grads, out_sem, k, e, slot).start()


def expert_kernel(n_first, p_all, x_all, dz_all, a_all, b_all, w1t, w3t, w2t, g1, g3, g2, part, h_all, da_all, db_all, dx_all, s1, s3, s2, out_sem):
    n_local, rows, n_tok = p_all.shape
    n_src, tok, _ = part.shape
    rows_in = (x_all, dz_all, h_all, da_all, db_all)
    stage = (s1, s3, s2)
    grads = (g1, g3, g2)

    def grad(k, e):
        weight_grad(rows_in, stage, grads, out_sem, k, e, e % N_STAGE, e - N_STAGE)

    def hidden(e):
        a = a_all[e].astype(F32)
        b = b_all[e].astype(F32)
        sg = jax.nn.sigmoid(a)
        silu = a * sg
        h_all[e] = (silu * b).astype(BF16)
        return b, sg, silu, 1.0 + a * (1.0 - sg)

    def middle(e, early=False):
        b, sg, silu, slope = hidden(e)
        if early:
            grad(2, e)
        dh = mm(dz_all[e], w2t[e], NN)
        da_all[e] = (dh * b * sg * slope).astype(BF16)
        db_all[e] = (dh * silu).astype(BF16)

    def back(e):
        dx_all[e] = (mm(da_all[e], w1t[e], NN) + mm(db_all[e], w3t[e], NN)).astype(BF16)

    middle(0, True)
    for e in range(n_local):
        if e in STEPS:
            for k in (2, 0, 1) if e else (0, 1):
                grad(k, STEPS.index(e))
        if e + 1 < n_local:
            middle(e + 1)
        back(e)
    total = mm(p_all[...].reshape(n_local * rows, n_tok), dx_all[...].reshape(n_local * rows, -1), TN)
    for s in range(n_src):
        part[s] = total[s * tok:(s + 1) * tok]
    for e in range(max(n_first - N_STAGE, 0), n_first):
        for k in range(3):
            grad_copy(stage, grads, out_sem, k, e, e % N_STAGE).wait()


def rest_kernel(n_first, x_all, dz_all, h_all, da_all, db_all, g1_in, g3_in, g2_in, g1, g3, g2, s1, s3, s2, out_sem):
    del g1_in, g3_in, g2_in
    n_local = x_all.shape[0]
    n_buf = s1.shape[0]
    stage = (s1, s3, s2)
    grads = (g1, g3, g2)
    rows_in = (x_all, dz_all, h_all, da_all, db_all)
    for e in range(n_first, n_local):
        for k in (2, 0, 1):
            weight_grad(rows_in, stage, grads, out_sem, k, e, (e - n_first) % n_buf, e - n_buf if e - n_buf >= n_first else -1)
    for e in range(max(n_first, n_local - n_buf), n_local):
        for k in range(3):
            grad_copy(stage, grads, out_sem, k, e, (e - n_first) % n_buf).wait()


def pair_kernel(part, mine_ref, theirs_ref, got, send_sem, recv_sem):
    ep, mate, far, far_mate = peers()
    entry_barrier((mate,))
    sends = []
    for k, owner in enumerate((far_mate, mate)):
        c = pltpu.make_async_remote_copy(src_ref=part.at[owner], dst_ref=got.at[k], send_sem=send_sem.at[k], recv_sem=recv_sem.at[k], device_id={'ep': mate}, device_id_type=MESH)
        c.start()
        sends.append(c)
    sends[0].wait_recv()
    theirs_ref[...] = part[far] + got[0]
    sends[1].wait_recv()
    mine_ref[...] = part[ep] + got[1]
    for c in sends:
        c.wait_send()


def solution(mesh):
    n_src = mesh.shape['ep']
    vmem = pl.BlockSpec(memory_space=pltpu.VMEM)
    hbm = pl.BlockSpec(memory_space=pltpu.HBM)

    def local_step(x_loc, dy_loc, ids_loc, gate_loc, slot_loc, w_gate, w_down, w_up):
        tok, top_k = ids_loc.shape
        n_local, d_model, ff = w_gate.shape
        n_exp = n_local * n_src
        cap = slot_capacity(tok, top_k, n_exp)
        rows = n_src * cap
        n_tok = n_src * tok
        dma = pltpu.SemaphoreType.DMA
        fixed = lambda v: pltpu.with_memory_space_constraint(v, pltpu.HBM)
        turned = tuple(pltpu.VMEM((n_local, w.shape[2], w.shape[1]), BF16) for w in (w_gate, w_up, w_down))
        p_all, x_all, dz_all, a_all, b_all, w1t, w3t, w2t = pl.pallas_call(
            functools.partial(gather_kernel, cap),
            out_shape=(
                pltpu.VMEM((n_local, rows, n_tok), BF16),
                pltpu.VMEM((n_local, rows, d_model), BF16),
                pltpu.VMEM((n_local, rows, d_model), BF16),
                pltpu.VMEM((n_local, rows, ff), BF16),
                pltpu.VMEM((n_local, rows, ff), BF16),
            ) + turned,
            in_specs=[hbm] * 8,
            out_specs=(vmem,) * 8,
            scratch_shapes=[
                pltpu.VMEM((n_tok, d_model), BF16),
                pltpu.VMEM((n_tok, d_model), BF16),
                pltpu.VMEM((n_src, 16, 128), F32),
                pltpu.VMEM((n_local, rows, 128), F32),
                pltpu.VMEM((top_k, tok), jnp.int32),
                pltpu.VMEM((top_k, tok), jnp.int32),
                pltpu.VMEM((top_k, tok), F32),
                pltpu.VMEM(w_gate.shape, BF16),
                pltpu.VMEM(w_up.shape, BF16),
                pltpu.VMEM((N_RING,) + w_down.shape[1:], BF16),
                dma((3, n_local)),
                dma((5,)),
                dma((15,)),
                dma((15,)),
            ],
            compiler_params=pltpu.CompilerParams(collective_id=0, has_side_effects=True, vmem_limit_bytes=25 << 20),
            name='gather',
        )(*map(fixed, (x_loc, dy_loc, ids_loc.T, slot_loc.T, gate_loc.T, w_gate, w_up, w_down)))
        grad_shapes = tuple(pltpu.HBM(w.shape, F32) for w in (w_gate, w_up, w_down))
        stage = lambda n: [pltpu.VMEM((n,) + w.shape[1:], F32) for w in (w_gate, w_up, w_down)]
        row_bytes = n_local * rows * (2 * d_model + 3 * ff) * 2
        g1, g3, g2, part, h_all, da_all, db_all = pl.pallas_call(
            functools.partial(expert_kernel, N_FIRST),
            out_shape=grad_shapes + (
                pltpu.VMEM((n_src, tok, d_model), F32),
                pltpu.VMEM((n_local, rows, ff), BF16),
                pltpu.VMEM((n_local, rows, ff), BF16),
                pltpu.VMEM((n_local, rows, ff), BF16),
            ),
            in_specs=[vmem] * 8,
            out_specs=(hbm,) * 3 + (vmem,) * 4,
            scratch_shapes=[pltpu.VMEM((n_local, rows, d_model), BF16), *stage(N_STAGE), dma((3, N_STAGE))],
            compiler_params=pltpu.CompilerParams(vmem_limit_bytes=20 << 20),
            name='experts',
        )(p_all, x_all, dz_all, a_all, b_all, w1t, w3t, w2t)
        rows_in = (x_all, dz_all, h_all, da_all, db_all)
        mine, theirs = pl.pallas_call(
            pair_kernel,
            out_shape=(pltpu.VMEM((tok, d_model), F32),) * 2,
            in_specs=[vmem],
            out_specs=(vmem,) * 2,
            scratch_shapes=[pltpu.VMEM((2, tok, d_model), F32), dma((2,)), dma((2,))],
            compiler_params=pltpu.CompilerParams(collective_id=1, has_side_effects=True, vmem_limit_bytes=4 << 20),
            name='pair',
        )(part)
        far = lax.ppermute(theirs, 'ep', [(i, (i + 2) % n_src) for i in range(n_src)])
        n_rest = n_local - N_FIRST
        g1, g3, g2 = pl.pallas_call(
            functools.partial(rest_kernel, N_FIRST),
            out_shape=grad_shapes,
            in_specs=[vmem] * 5 + [hbm] * 3,
            out_specs=(hbm,) * 3,
            scratch_shapes=[*stage(N_BUF), dma((3, N_BUF))],
            input_output_aliases={5: 0, 6: 1, 7: 2},
            compiler_params=pltpu.CompilerParams(vmem_limit_bytes=20 << 20),
            cost_estimate=pl.CostEstimate(flops=2 * 3 * n_rest * rows * d_model * ff, bytes_accessed=n_rest * 3 * d_model * ff * 4 + row_bytes, transcendentals=0),
            name='rest',
        )(*rows_in, g1, g3, g2)
        dx_loc = (mine + far).astype(BF16)
        return dx_loc, g1, g2, g3

    tok_spec = P(('dp', 'ep'), None)
    w_spec = P('ep', None, None)
    grad_spec = P(('dp', 'ep'), None, None)
    return jax.shard_map(local_step, mesh=mesh, in_specs=(tok_spec, tok_spec, tok_spec, tok_spec, tok_spec, w_spec, w_spec, w_spec), out_specs=(tok_spec, grad_spec, grad_spec, grad_spec), check_vma=False)
```

```python
import functools

import jax
import jax.numpy as jnp
from jax import lax
from jax.experimental import pallas as pl
from jax.experimental.pallas import tpu as pltpu
from jax.sharding import PartitionSpec as P

MESH = pl.DeviceIdType.MESH
F32 = jnp.float32
BF16 = jnp.bfloat16
NN = (((1,), (0,)), ((), ()))
NT = (((1,), (1,)), ((), ()))
TN = (((0,), (0,)), ((), ()))
N_FIRST = 5
N_BUF = 3
N_STAGE = 2
TAIL_ROWS = 16
N_RING = 6
U_ROUTE = 2
U_PAIR = 4
STEPS = (0, 1, 2, 4, 5)


def slot_capacity(tok_dev, top_k, n_exp):
    return ((3 * tok_dev * top_k) // (2 * n_exp) + 7) // 8 * 8


def mm(a, b, dims):
    return lax.dot_general(a, b, dims, preferred_element_type=F32)


def peers():
    ep = lax.axis_index('ep')
    core = lax.rem(ep, 2)
    chip = ep - core
    mate = chip + 1 - core
    far = lax.rem(ep + 2, 4)
    far_mate = lax.rem(mate + 2, 4)
    return ep, mate, far, far_mate


def entry_barrier(others):
    barrier = pltpu.get_barrier_semaphore()
    for other in others:
        pl.semaphore_signal(barrier, inc=1, device_id={'ep': other}, device_id_type=MESH)
    pl.semaphore_wait(barrier, len(others))


def run(lo, hi, body, unroll):
    def step(e, carry):
        body(e)
        return carry

    if unroll == 0:
        for e in range(lo, hi):
            body(e)
    else:
        lax.fori_loop(lo, hi, step, 0, unroll=unroll)


def gather_kernel(cap, x_hbm, dy_hbm, ids_hbm, slot_hbm, gate_hbm, w1_hbm, w3_hbm, w2_hbm, p_all, x_all, dz_all, a_all, b_all, w1t, w3t, w2t, xg, dyg, metag, g_rows, ids_ref, slot_ref, gate_ref, w1, w3, w2, w_sem, loc_sem, send_sem, recv_sem):
    ep, mate, far, far_mate = peers()
    n_local, rows, n_tok = p_all.shape
    n_src = metag.shape[0]
    tok = n_tok // n_src
    barrier = pltpu.get_barrier_semaphore()
    for other in (mate, far, far_mate):
        pl.semaphore_signal(barrier, inc=1, device_id={'ep': other}, device_id_type=MESH)
    mine = pl.multiple_of(ep * tok, tok)
    theirs = pl.multiple_of(far * tok, tok)
    small = []
    for k, (src, dst) in enumerate(((x_hbm, xg.at[pl.ds(mine, tok)]), (dy_hbm, dyg.at[pl.ds(mine, tok)]), (ids_hbm, ids_ref), (slot_hbm, slot_ref), (gate_hbm, gate_ref))):
        c = pltpu.make_async_copy(src, dst, loc_sem.at[k])
        c.start()
        small.append(c)

    n_ring = w2.shape[0]

    def load_w2(e):
        return pltpu.make_async_copy(w2_hbm.at[e], w2.at[lax.rem(e, n_ring)], w_sem.at[2, e])

    def loads(e):
        return [pltpu.make_async_copy(src.at[e], dst.at[e], w_sem.at[k, e]) for k, (src, dst) in enumerate(((w1_hbm, w1), (w3_hbm, w3)))]

    for e in range(n_local):
        for c in loads(e):
            c.start(priority=1)
        if e < n_ring:
            load_w2(e).start(priority=1)
    for c in small:
        c.wait()
    key = jnp.where(slot_ref[...] >= 0, ids_ref[...] * cap + slot_ref[...], -1)
    metag[ep, 0:8, 0:tok] = key.astype(F32)
    metag[ep, 8:16, 0:tok] = gate_ref[...]
    metag[ep, 0:8, tok:2 * tok] = jnp.zeros((8, tok), F32)
    metag[ep, 8:16, tok:2 * tok] = jnp.zeros((8, tok), F32)
    pl.semaphore_wait(barrier, 3)

    def send(src, dst, k, to):
        c = pltpu.make_async_remote_copy(src_ref=src, dst_ref=dst, send_sem=send_sem.at[k], recv_sem=recv_sem.at[k], device_id={'ep': to}, device_id_type=MESH)
        c.start()
        return c

    half = tok // 2
    tail = TAIL_ROWS
    pieces = [(xg, 0, half), (xg, half, half), (dyg, 0, tok - tail), (dyg, tok - tail, tail)]

    def block(k, base):
        ref, off, size = pieces[k]
        return ref.at[pl.ds(base + off, size)]

    metas = [send(metag.at[ep], metag.at[ep], 12 + k, to) for k, to in enumerate((far, mate, far_mate))]
    to_far = [send(block(k, mine), block(k, mine), k, far) for k in range(4)]
    direct = send(block(3, mine), block(3, mine), 11, far_mate)
    relays = []
    to_mate = [send(block(k, mine), block(k, mine), 4 + k, mate) for k in range(4)]

    def ready(e):
        for c in loads(e):
            c.wait()
        load_w2(e).wait()

    def flip(e):
        w1t[e] = w1[e].T
        w3t[e] = w3[e].T
        slot = lax.rem(e, n_ring)
        w2t[e] = w2[slot].T

    def turn(e):
        ready(e)
        flip(e)

    def relay(k):
        to_far[k].wait_recv()
        relays.append(send(block(k, theirs), block(k, theirs), 8 + k, mate))

    def turn_load(e):
        turn(e)
        load_w2(e + n_ring).start(priority=1)

    run(0, n_local - n_ring, turn_load, 1)
    run(n_local - n_ring, 4, turn, 1)
    for c in metas:
        c.wait_recv()
    lane = lax.broadcasted_iota(jnp.int32, (1, n_tok), 1)
    src_base = (lane // tok) * cap
    row_id = lax.broadcasted_iota(jnp.int32, (rows, n_tok), 0)
    meta = all_meta(metag, tok)
    key = meta[0:8, :].astype(jnp.int32)
    gate = meta[8:16, :]

    def route(e):
        lo = (ep * n_local + e) * cap
        hit = (key >= lo) & (key < lo + cap)
        slot = jnp.sum(jnp.where(hit, key - lo + 1, 0), axis=0, keepdims=True)
        g_tok = jnp.sum(jnp.where(hit, gate, 0.0), axis=0, keepdims=True)
        pick = row_id == jnp.where(slot > 0, slot - 1 + src_base, -1)
        p_all[e] = jnp.where(pick, 1.0, 0.0).astype(BF16)
        g_rows[e] = jnp.broadcast_to(jnp.sum(jnp.where(pick, g_tok, 0.0), axis=1, keepdims=True), g_rows.shape[1:])

    turn(4)
    relay(0)
    relay(1)
    ready(5)
    for e in range(n_local):
        route(e)
    flip(5)
    for c in to_mate[:2] + relays[:2]:
        c.wait_recv()

    def spread(i):
        two = pl.ds(i * 2, 2)
        x_all[two] = mm(p_all[two].reshape(2 * rows, n_tok), xg[...], NN).astype(BF16).reshape(2, rows, -1)

    def front(e):
        a_all[e] = mm(x_all[e], w1[e], NN).astype(BF16)
        b_all[e] = mm(x_all[e], w3[e], NN).astype(BF16)

    ready(6)
    for i in range(n_local // 2):
        spread(i)
    front(0)
    flip(6)
    front(1)
    relay(2)
    relays.append(direct)
    ready(7)
    front(2)
    flip(7)
    for e in range(3, n_local):
        front(e)
    for c in to_mate[2:] + relays[2:] + to_far[3:]:
        c.wait_recv()

    def scale(i):
        two = pl.ds(i * 2, 2)
        dy_rows = mm(p_all[two].reshape(2 * rows, n_tok), dyg[...], NN).reshape(2, rows, -1)
        dz_all[two] = (g_rows[two][:, :, 0:1] * dy_rows).astype(BF16)

    run(0, n_local // 2, scale, U_PAIR)
    for c in to_far + to_mate + relays + metas:
        c.wait_send()


def all_meta(metag, tok):
    halves = []
    for pair in range(metag.shape[0] // 2):
        halves.append(metag[2 * pair] + pltpu.roll(metag[2 * pair + 1], tok, 1))
    return jnp.concatenate(halves, axis=1)


def grad_copy(stage, grads, out_sem, k, e, slot):
    return pltpu.make_async_copy(stage[k].at[slot], grads[k].at[e], out_sem.at[k, slot])


def weight_grad(rows_in, stage, grads, out_sem, k, e, slot, prev):
    x_all, dz_all, h_all, da_all, db_all = rows_in
    if prev >= 0:
        grad_copy(stage, grads, out_sem, k, prev, slot).wait()
    left, right = ((x_all, da_all), (x_all, db_all), (h_all, dz_all))[k]
    stage[k][slot] = mm(left[e], right[e], TN)
    grad_copy(stage, grads, out_sem, k, e, slot).start()


def expert_kernel(n_first, p_all, x_all, dz_all, a_all, b_all, w1t, w3t, w2t, g1, g3, g2, part, h_all, da_all, db_all, dx_all, s1, s3, s2, out_sem):
    n_local, rows, n_tok = p_all.shape
    n_src, tok, _ = part.shape
    rows_in = (x_all, dz_all, h_all, da_all, db_all)
    stage = (s1, s3, s2)
    grads = (g1, g3, g2)

    def grad(k, e):
        weight_grad(rows_in, stage, grads, out_sem, k, e, e % N_STAGE, e - N_STAGE)

    def hidden(e):
        a = a_all[e].astype(F32)
        b = b_all[e].astype(F32)
        sg = jax.nn.sigmoid(a)
        silu = a * sg
        h_all[e] = (silu * b).astype(BF16)
        return b, sg, silu, 1.0 + a * (1.0 - sg)

    def middle(e, early=False):
        b, sg, silu, slope = hidden(e)
        if early:
            grad(2, e)
        dh = mm(dz_all[e], w2t[e], NN)
        da_all[e] = (dh * b * sg * slope).astype(BF16)
        db_all[e] = (dh * silu).astype(BF16)

    def back(e):
        dx_all[e] = (mm(da_all[e], w1t[e], NN) + mm(db_all[e], w3t[e], NN)).astype(BF16)

    middle(0, True)
    for e in range(n_local):
        if e in STEPS:
            for k in (2, 0, 1) if e else (0, 1):
                grad(k, STEPS.index(e))
        if e + 1 < n_local:
            middle(e + 1)
        back(e)
    total = mm(p_all[...].reshape(n_local * rows, n_tok), dx_all[...].reshape(n_local * rows, -1), TN)
    for s in range(n_src):
        part[s] = total[s * tok:(s + 1) * tok]
    for e in range(max(n_first - N_STAGE, 0), n_first):
        for k in range(3):
            grad_copy(stage, grads, out_sem, k, e, e % N_STAGE).wait()


def rest_kernel(n_first, x_all, dz_all, h_all, da_all, db_all, g1_in, g3_in, g2_in, g1, g3, g2, s1, s3, s2, out_sem):
    del g1_in, g3_in, g2_in
    n_local = x_all.shape[0]
    n_buf = s1.shape[0]
    stage = (s1, s3, s2)
    grads = (g1, g3, g2)
    rows_in = (x_all, dz_all, h_all, da_all, db_all)
    for e in range(n_first, n_local):
        for k in (2, 0, 1):
            weight_grad(rows_in, stage, grads, out_sem, k, e, (e - n_first) % n_buf, e - n_buf if e - n_buf >= n_first else -1)
    for e in range(max(n_first, n_local - n_buf), n_local):
        for k in range(3):
            grad_copy(stage, grads, out_sem, k, e, (e - n_first) % n_buf).wait()


def pair_kernel(part, mine_ref, theirs_ref, got, send_sem, recv_sem):
    ep, mate, far, far_mate = peers()
    entry_barrier((mate,))
    sends = []
    for k, owner in enumerate((far_mate, mate)):
        c = pltpu.make_async_remote_copy(src_ref=part.at[owner], dst_ref=got.at[k], send_sem=send_sem.at[k], recv_sem=recv_sem.at[k], device_id={'ep': mate}, device_id_type=MESH)
        c.start()
        sends.append(c)
    sends[0].wait_recv()
    theirs_ref[...] = part[far] + got[0]
    sends[1].wait_recv()
    mine_ref[...] = part[ep] + got[1]
    for c in sends:
        c.wait_send()


def solution(mesh):
    n_src = mesh.shape['ep']
    vmem = pl.BlockSpec(memory_space=pltpu.VMEM)
    hbm = pl.BlockSpec(memory_space=pltpu.HBM)

    def local_step(x_loc, dy_loc, ids_loc, gate_loc, slot_loc, w_gate, w_down, w_up):
        tok, top_k = ids_loc.shape
        n_local, d_model, ff = w_gate.shape
        n_exp = n_local * n_src
        cap = slot_capacity(tok, top_k, n_exp)
        rows = n_src * cap
        n_tok = n_src * tok
        dma = pltpu.SemaphoreType.DMA
        fixed = lambda v: pltpu.with_memory_space_constraint(v, pltpu.HBM)
        turned = tuple(pltpu.VMEM((n_local, w.shape[2], w.shape[1]), BF16) for w in (w_gate, w_up, w_down))
        p_all, x_all, dz_all, a_all, b_all, w1t, w3t, w2t = pl.pallas_call(
            functools.partial(gather_kernel, cap),
            out_shape=(
                pltpu.VMEM((n_local, rows, n_tok), BF16),
                pltpu.VMEM((n_local, rows, d_model), BF16),
                pltpu.VMEM((n_local, rows, d_model), BF16),
                pltpu.VMEM((n_local, rows, ff), BF16),
                pltpu.VMEM((n_local, rows, ff), BF16),
            ) + turned,
            in_specs=[hbm] * 8,
            out_specs=(vmem,) * 8,
            scratch_shapes=[
                pltpu.VMEM((n_tok, d_model), BF16),
                pltpu.VMEM((n_tok, d_model), BF16),
                pltpu.VMEM((n_src, 16, 128), F32),
                pltpu.VMEM((n_local, rows, 128), F32),
                pltpu.VMEM((top_k, tok), jnp.int32),
                pltpu.VMEM((top_k, tok), jnp.int32),
                pltpu.VMEM((top_k, tok), F32),
                pltpu.VMEM(w_gate.shape, BF16),
                pltpu.VMEM(w_up.shape, BF16),
                pltpu.VMEM((N_RING,) + w_down.shape[1:], BF16),
                dma((3, n_local)),
                dma((5,)),
                dma((15,)),
                dma((15,)),
            ],
            compiler_params=pltpu.CompilerParams(collective_id=0, has_side_effects=True, vmem_limit_bytes=25 << 20),
            name='gather',
        )(*map(fixed, (x_loc, dy_loc, ids_loc.T, slot_loc.T, gate_loc.T, w_gate, w_up, w_down)))
        grad_shapes = tuple(pltpu.HBM(w.shape, F32) for w in (w_gate, w_up, w_down))
        stage = lambda n: [pltpu.VMEM((n,) + w.shape[1:], F32) for w in (w_gate, w_up, w_down)]
        row_bytes = n_local * rows * (2 * d_model + 3 * ff) * 2
        g1, g3, g2, part, h_all, da_all, db_all = pl.pallas_call(
            functools.partial(expert_kernel, N_FIRST),
            out_shape=grad_shapes + (
                pltpu.VMEM((n_src, tok, d_model), F32),
                pltpu.VMEM((n_local, rows, ff), BF16),
                pltpu.VMEM((n_local, rows, ff), BF16),
                pltpu.VMEM((n_local, rows, ff), BF16),
            ),
            in_specs=[vmem] * 8,
            out_specs=(hbm,) * 3 + (vmem,) * 4,
            scratch_shapes=[pltpu.VMEM((n_local, rows, d_model), BF16), *stage(N_STAGE), dma((3, N_STAGE))],
            compiler_params=pltpu.CompilerParams(vmem_limit_bytes=20 << 20),
            name='experts',
        )(p_all, x_all, dz_all, a_all, b_all, w1t, w3t, w2t)
        rows_in = (x_all, dz_all, h_all, da_all, db_all)
        mine, theirs = pl.pallas_call(
            pair_kernel,
            out_shape=(pltpu.VMEM((tok, d_model), F32),) * 2,
            in_specs=[vmem],
            out_specs=(vmem,) * 2,
            scratch_shapes=[pltpu.VMEM((2, tok, d_model), F32), dma((2,)), dma((2,))],
            compiler_params=pltpu.CompilerParams(collective_id=1, has_side_effects=True, vmem_limit_bytes=4 << 20),
            name='pair',
        )(part)
        far = lax.ppermute(theirs, 'ep', [(i, (i + 2) % n_src) for i in range(n_src)])
        n_rest = n_local - N_FIRST
        g1, g3, g2 = pl.pallas_call(
            functools.partial(rest_kernel, N_FIRST),
            out_shape=grad_shapes,
            in_specs=[vmem] * 5 + [hbm] * 3,
            out_specs=(hbm,) * 3,
            scratch_shapes=[*stage(N_BUF), dma((3, N_BUF))],
            input_output_aliases={5: 0, 6: 1, 7: 2},
            compiler_params=pltpu.CompilerParams(vmem_limit_bytes=20 << 20),
            cost_estimate=pl.CostEstimate(flops=2 * 3 * n_rest * rows * d_model * ff, bytes_accessed=n_rest * 3 * d_model * ff * 4 + row_bytes, transcendentals=0),
            name='rest',
        )(*rows_in, g1, g3, g2)
        dx_loc = (mine + far).astype(BF16)
        return dx_loc, g1, g2, g3

    tok_spec = P(('dp', 'ep'), None)
    w_spec = P('ep', None, None)
    grad_spec = P(('dp', 'ep'), None, None)
    return jax.shard_map(local_step, mesh=mesh, in_specs=(tok_spec, tok_spec, tok_spec, tok_spec, tok_spec, w_spec, w_spec, w_spec), out_specs=(tok_spec, grad_spec, grad_spec, grad_spec), check_vma=False)
```

```python
import functools

import jax
import jax.numpy as jnp
from jax import lax
from jax.experimental import pallas as pl
from jax.experimental.pallas import tpu as pltpu
from jax.sharding import PartitionSpec as P

MESH = pl.DeviceIdType.MESH
F32 = jnp.float32
BF16 = jnp.bfloat16
NN = (((1,), (0,)), ((), ()))
NT = (((1,), (1,)), ((), ()))
TN = (((0,), (0,)), ((), ()))
N_FIRST = 5
N_BUF = 3
N_STAGE = 2
TAIL_ROWS = 16
N_RING = 6
U_ROUTE = 2
U_PAIR = 4
STEPS = (0, 1, 2, 4, 5)


def slot_capacity(tok_dev, top_k, n_exp):
    return ((3 * tok_dev * top_k) // (2 * n_exp) + 7) // 8 * 8


def mm(a, b, dims):
    return lax.dot_general(a, b, dims, preferred_element_type=F32)


def peers():
    ep = lax.axis_index('ep')
    core = lax.rem(ep, 2)
    chip = ep - core
    mate = chip + 1 - core
    far = lax.rem(ep + 2, 4)
    far_mate = lax.rem(mate + 2, 4)
    return ep, mate, far, far_mate


def entry_barrier(others):
    barrier = pltpu.get_barrier_semaphore()
    for other in others:
        pl.semaphore_signal(barrier, inc=1, device_id={'ep': other}, device_id_type=MESH)
    pl.semaphore_wait(barrier, len(others))


def run(lo, hi, body, unroll):
    def step(e, carry):
        body(e)
        return carry

    if unroll == 0:
        for e in range(lo, hi):
            body(e)
    else:
        lax.fori_loop(lo, hi, step, 0, unroll=unroll)


def gather_kernel(cap, x_hbm, dy_hbm, ids_hbm, slot_hbm, gate_hbm, w1_hbm, w3_hbm, w2_hbm, p_all, x_all, dz_all, a_all, b_all, w1t, w3t, w2t, xg, dyg, metag, g_rows, ids_ref, slot_ref, gate_ref, w1, w3, w2, w_sem, loc_sem, send_sem, recv_sem):
    ep, mate, far, far_mate = peers()
    n_local, rows, n_tok = p_all.shape
    n_src = metag.shape[0]
    tok = n_tok // n_src
    barrier = pltpu.get_barrier_semaphore()
    for other in (mate, far, far_mate):
        pl.semaphore_signal(barrier, inc=1, device_id={'ep': other}, device_id_type=MESH)
    mine = pl.multiple_of(ep * tok, tok)
    theirs = pl.multiple_of(far * tok, tok)
    small = []
    for k, (src, dst) in enumerate(((x_hbm, xg.at[pl.ds(mine, tok)]), (dy_hbm, dyg.at[pl.ds(mine, tok)]), (ids_hbm, ids_ref), (slot_hbm, slot_ref), (gate_hbm, gate_ref))):
        c = pltpu.make_async_copy(src, dst, loc_sem.at[k])
        c.start()
        small.append(c)

    n_ring = w2.shape[0]

    def load_w2(e):
        return pltpu.make_async_copy(w2_hbm.at[e], w2.at[lax.rem(e, n_ring)], w_sem.at[2, e])

    def loads(e):
        return [pltpu.make_async_copy(src.at[e], dst.at[e], w_sem.at[k, e]) for k, (src, dst) in enumerate(((w1_hbm, w1), (w3_hbm, w3)))]

    for e in range(n_local):
        for c in loads(e):
            c.start(priority=1)
        if e < n_ring:
            load_w2(e).start(priority=1)
    for c in small:
        c.wait()
    key = jnp.where(slot_ref[...] >= 0, ids_ref[...] * cap + slot_ref[...], -1)
    metag[ep, 0:8, 0:tok] = key.astype(F32)
    metag[ep, 8:16, 0:tok] = gate_ref[...]
    metag[ep, 0:8, tok:2 * tok] = jnp.zeros((8, tok), F32)
    metag[ep, 8:16, tok:2 * tok] = jnp.zeros((8, tok), F32)
    pl.semaphore_wait(barrier, 3)

    def send(src, dst, k, to):
        c = pltpu.make_async_remote_copy(src_ref=src, dst_ref=dst, send_sem=send_sem.at[k], recv_sem=recv_sem.at[k], device_id={'ep': to}, device_id_type=MESH)
        c.start()
        return c

    half = tok // 2
    tail = TAIL_ROWS
    pieces = [(xg, 0, half), (xg, half, half), (dyg, 0, tok - tail), (dyg, tok - tail, tail)]

    def block(k, base):
        ref, off, size = pieces[k]
        return ref.at[pl.ds(base + off, size)]

    metas = [send(metag.at[ep], metag.at[ep], 12 + k, to) for k, to in enumerate((far, mate, far_mate))]
    to_far = [send(block(k, mine), block(k, mine), k, far) for k in range(4)]
    direct = send(block(3, mine), block(3, mine), 11, far_mate)
    relays = []
    to_mate = [send(block(k, mine), block(k, mine), 4 + k, mate) for k in range(4)]

    def ready(e):
        for c in loads(e):
            c.wait()
        load_w2(e).wait()

    def flip(e):
        w1t[e] = w1[e].T
        w3t[e] = w3[e].T
        slot = lax.rem(e, n_ring)
        w2t[e] = w2[slot].T

    def turn(e):
        ready(e)
        flip(e)

    def relay(k):
        to_far[k].wait_recv()
        relays.append(send(block(k, theirs), block(k, theirs), 8 + k, mate))

    def turn_load(e):
        turn(e)
        load_w2(e + n_ring).start(priority=1)

    run(0, n_local - n_ring, turn_load, 1)
    run(n_local - n_ring, 4, turn, 1)
    for c in metas:
        c.wait_recv()
    lane = lax.broadcasted_iota(jnp.int32, (1, n_tok), 1)
    src_base = (lane // tok) * cap
    row_id = lax.broadcasted_iota(jnp.int32, (rows, n_tok), 0)
    meta = all_meta(metag, tok)
    key = meta[0:8, :].astype(jnp.int32)
    gate = meta[8:16, :]

    def route(e):
        lo = (ep * n_local + e) * cap
        hit = (key >= lo) & (key < lo + cap)
        slot = jnp.sum(jnp.where(hit, key - lo + 1, 0), axis=0, keepdims=True)
        g_tok = jnp.sum(jnp.where(hit, gate, 0.0), axis=0, keepdims=True)
        pick = row_id == jnp.where(slot > 0, slot - 1 + src_base, -1)
        p_all[e] = jnp.where(pick, 1.0, 0.0).astype(BF16)
        g_rows[e] = jnp.broadcast_to(jnp.sum(jnp.where(pick, g_tok, 0.0), axis=1, keepdims=True), g_rows.shape[1:])

    turn(4)
    relay(0)
    relay(1)
    ready(5)
    for e in range(n_local):
        route(e)
    flip(5)
    for c in to_mate[:2] + relays[:2]:
        c.wait_recv()

    def spread(i):
        two = pl.ds(i * 2, 2)
        x_all[two] = mm(p_all[two].reshape(2 * rows, n_tok), xg[...], NN).astype(BF16).reshape(2, rows, -1)

    def front(e):
        a_all[e] = mm(x_all[e], w1[e], NN).astype(BF16)
        b_all[e] = mm(x_all[e], w3[e], NN).astype(BF16)

    ready(6)
    for i in range(n_local // 2):
        spread(i)
    front(0)
    flip(6)
    front(1)
    relay(2)
    relays.append(direct)
    ready(7)
    front(2)
    flip(7)
    for e in range(3, 6):
        front(e)
    for c in to_mate[2:] + relays[2:] + to_far[3:]:
        c.wait_recv()

    def scale(i):
        two = pl.ds(i * 2, 2)
        dy_rows = mm(p_all[two].reshape(2 * rows, n_tok), dyg[...], NN).reshape(2, rows, -1)
        dz_all[two] = (g_rows[two][:, :, 0:1] * dy_rows).astype(BF16)

    for i in range(n_local // 2):
        scale(i)
        if 6 + i < n_local:
            front(6 + i)
    for c in to_far + to_mate + relays + metas:
        c.wait_send()


def all_meta(metag, tok):
    halves = []
    for pair in range(metag.shape[0] // 2):
        halves.append(metag[2 * pair] + pltpu.roll(metag[2 * pair + 1], tok, 1))
    return jnp.concatenate(halves, axis=1)


def grad_copy(stage, grads, out_sem, k, e, slot):
    return pltpu.make_async_copy(stage[k].at[slot], grads[k].at[e], out_sem.at[k, slot])


def weight_grad(rows_in, stage, grads, out_sem, k, e, slot, prev):
    x_all, dz_all, h_all, da_all, db_all = rows_in
    if prev >= 0:
        grad_copy(stage, grads, out_sem, k, prev, slot).wait()
    left, right = ((x_all, da_all), (x_all, db_all), (h_all, dz_all))[k]
    stage[k][slot] = mm(left[e], right[e], TN)
    grad_copy(stage, grads, out_sem, k, e, slot).start()


def expert_kernel(n_first, p_all, x_all, dz_all, a_all, b_all, w1t, w3t, w2t, g1, g3, g2, part, h_all, da_all, db_all, dx_all, s1, s3, s2, out_sem):
    n_local, rows, n_tok = p_all.shape
    n_src, tok, _ = part.shape
    rows_in = (x_all, dz_all, h_all, da_all, db_all)
    stage = (s1, s3, s2)
    grads = (g1, g3, g2)

    def grad(k, e):
        weight_grad(rows_in, stage, grads, out_sem, k, e, e % N_STAGE, e - N_STAGE)

    def hidden(e):
        a = a_all[e].astype(F32)
        b = b_all[e].astype(F32)
        sg = jax.nn.sigmoid(a)
        silu = a * sg
        h_all[e] = (silu * b).astype(BF16)
        return b, sg, silu, 1.0 + a * (1.0 - sg)

    def middle(e, early=False):
        b, sg, silu, slope = hidden(e)
        if early:
            grad(2, e)
        dh = mm(dz_all[e], w2t[e], NN)
        da_all[e] = (dh * b * sg * slope).astype(BF16)
        db_all[e] = (dh * silu).astype(BF16)

    def back(e):
        dx_all[e] = (mm(da_all[e], w1t[e], NN) + mm(db_all[e], w3t[e], NN)).astype(BF16)

    middle(0, True)
    for e in range(n_local):
        if e in STEPS:
            for k in (2, 0, 1) if e else (0, 1):
                grad(k, STEPS.index(e))
        if e + 1 < n_local:
            middle(e + 1)
        back(e)
    total = mm(p_all[...].reshape(n_local * rows, n_tok), dx_all[...].reshape(n_local * rows, -1), TN)
    for s in range(n_src):
        part[s] = total[s * tok:(s + 1) * tok]
    for e in range(max(n_first - N_STAGE, 0), n_first):
        for k in range(3):
            grad_copy(stage, grads, out_sem, k, e, e % N_STAGE).wait()


def rest_kernel(n_first, x_all, dz_all, h_all, da_all, db_all, g1_in, g3_in, g2_in, g1, g3, g2, s1, s3, s2, out_sem):
    del g1_in, g3_in, g2_in
    n_local = x_all.shape[0]
    n_buf = s1.shape[0]
    stage = (s1, s3, s2)
    grads = (g1, g3, g2)
    rows_in = (x_all, dz_all, h_all, da_all, db_all)
    for e in range(n_first, n_local):
        for k in (2, 0, 1):
            weight_grad(rows_in, stage, grads, out_sem, k, e, (e - n_first) % n_buf, e - n_buf if e - n_buf >= n_first else -1)
    for e in range(max(n_first, n_local - n_buf), n_local):
        for k in range(3):
            grad_copy(stage, grads, out_sem, k, e, (e - n_first) % n_buf).wait()


def pair_kernel(part, mine_ref, theirs_ref, got, send_sem, recv_sem):
    ep, mate, far, far_mate = peers()
    entry_barrier((mate,))
    sends = []
    for k, owner in enumerate((far_mate, mate)):
        c = pltpu.make_async_remote_copy(src_ref=part.at[owner], dst_ref=got.at[k], send_sem=send_sem.at[k], recv_sem=recv_sem.at[k], device_id={'ep': mate}, device_id_type=MESH)
        c.start()
        sends.append(c)
    sends[0].wait_recv()
    theirs_ref[...] = part[far] + got[0]
    sends[1].wait_recv()
    mine_ref[...] = part[ep] + got[1]
    for c in sends:
        c.wait_send()


def solution(mesh):
    n_src = mesh.shape['ep']
    vmem = pl.BlockSpec(memory_space=pltpu.VMEM)
    hbm = pl.BlockSpec(memory_space=pltpu.HBM)

    def local_step(x_loc, dy_loc, ids_loc, gate_loc, slot_loc, w_gate, w_down, w_up):
        tok, top_k = ids_loc.shape
        n_local, d_model, ff = w_gate.shape
        n_exp = n_local * n_src
        cap = slot_capacity(tok, top_k, n_exp)
        rows = n_src * cap
        n_tok = n_src * tok
        dma = pltpu.SemaphoreType.DMA
        fixed = lambda v: pltpu.with_memory_space_constraint(v, pltpu.HBM)
        turned = tuple(pltpu.VMEM((n_local, w.shape[2], w.shape[1]), BF16) for w in (w_gate, w_up, w_down))
        p_all, x_all, dz_all, a_all, b_all, w1t, w3t, w2t = pl.pallas_call(
            functools.partial(gather_kernel, cap),
            out_shape=(
                pltpu.VMEM((n_local, rows, n_tok), BF16),
                pltpu.VMEM((n_local, rows, d_model), BF16),
                pltpu.VMEM((n_local, rows, d_model), BF16),
                pltpu.VMEM((n_local, rows, ff), BF16),
                pltpu.VMEM((n_local, rows, ff), BF16),
            ) + turned,
            in_specs=[hbm] * 8,
            out_specs=(vmem,) * 8,
            scratch_shapes=[
                pltpu.VMEM((n_tok, d_model), BF16),
                pltpu.VMEM((n_tok, d_model), BF16),
                pltpu.VMEM((n_src, 16, 128), F32),
                pltpu.VMEM((n_local, rows, 128), F32),
                pltpu.VMEM((top_k, tok), jnp.int32),
                pltpu.VMEM((top_k, tok), jnp.int32),
                pltpu.VMEM((top_k, tok), F32),
                pltpu.VMEM(w_gate.shape, BF16),
                pltpu.VMEM(w_up.shape, BF16),
                pltpu.VMEM((N_RING,) + w_down.shape[1:], BF16),
                dma((3, n_local)),
                dma((5,)),
                dma((15,)),
                dma((15,)),
            ],
            compiler_params=pltpu.CompilerParams(collective_id=0, has_side_effects=True, vmem_limit_bytes=25 << 20),
            name='gather',
        )(*map(fixed, (x_loc, dy_loc, ids_loc.T, slot_loc.T, gate_loc.T, w_gate, w_up, w_down)))
        grad_shapes = tuple(pltpu.HBM(w.shape, F32) for w in (w_gate, w_up, w_down))
        stage = lambda n: [pltpu.VMEM((n,) + w.shape[1:], F32) for w in (w_gate, w_up, w_down)]
        row_bytes = n_local * rows * (2 * d_model + 3 * ff) * 2
        g1, g3, g2, part, h_all, da_all, db_all = pl.pallas_call(
            functools.partial(expert_kernel, N_FIRST),
            out_shape=grad_shapes + (
                pltpu.VMEM((n_src, tok, d_model), F32),
                pltpu.VMEM((n_local, rows, ff), BF16),
                pltpu.VMEM((n_local, rows, ff), BF16),
                pltpu.VMEM((n_local, rows, ff), BF16),
            ),
            in_specs=[vmem] * 8,
            out_specs=(hbm,) * 3 + (vmem,) * 4,
            scratch_shapes=[pltpu.VMEM((n_local, rows, d_model), BF16), *stage(N_STAGE), dma((3, N_STAGE))],
            compiler_params=pltpu.CompilerParams(vmem_limit_bytes=20 << 20),
            name='experts',
        )(p_all, x_all, dz_all, a_all, b_all, w1t, w3t, w2t)
        rows_in = (x_all, dz_all, h_all, da_all, db_all)
        mine, theirs = pl.pallas_call(
            pair_kernel,
            out_shape=(pltpu.VMEM((tok, d_model), F32),) * 2,
            in_specs=[vmem],
            out_specs=(vmem,) * 2,
            scratch_shapes=[pltpu.VMEM((2, tok, d_model), F32), dma((2,)), dma((2,))],
            compiler_params=pltpu.CompilerParams(collective_id=1, has_side_effects=True, vmem_limit_bytes=4 << 20),
            name='pair',
        )(part)
        far = lax.ppermute(theirs, 'ep', [(i, (i + 2) % n_src) for i in range(n_src)])
        n_rest = n_local - N_FIRST
        g1, g3, g2 = pl.pallas_call(
            functools.partial(rest_kernel, N_FIRST),
            out_shape=grad_shapes,
            in_specs=[vmem] * 5 + [hbm] * 3,
            out_specs=(hbm,) * 3,
            scratch_shapes=[*stage(N_BUF), dma((3, N_BUF))],
            input_output_aliases={5: 0, 6: 1, 7: 2},
            compiler_params=pltpu.CompilerParams(vmem_limit_bytes=20 << 20),
            cost_estimate=pl.CostEstimate(flops=2 * 3 * n_rest * rows * d_model * ff, bytes_accessed=n_rest * 3 * d_model * ff * 4 + row_bytes, transcendentals=0),
            name='rest',
        )(*rows_in, g1, g3, g2)
        dx_loc = (mine + far).astype(BF16)
        return dx_loc, g1, g2, g3

    tok_spec = P(('dp', 'ep'), None)
    w_spec = P('ep', None, None)
    grad_spec = P(('dp', 'ep'), None, None)
    return jax.shard_map(local_step, mesh=mesh, in_specs=(tok_spec, tok_spec, tok_spec, tok_spec, tok_spec, w_spec, w_spec, w_spec), out_specs=(tok_spec, grad_spec, grad_spec, grad_spec), check_vma=False)
```
